32 devices in a mesh: gx: 4 (over x, core), gy: 4 (over z), row: 2 (over y).
Axes of the slice: x: 2, y: 2, z: 4, core: 2. Of those that a mesh axis runs over, the one named last changes fastest.
Arguments:
- concentrations: float32 [2, 64, 128, 256], P(None, 'gx', 'gy', 'row'), may hold values from 0 to 1
- diffusivity: float32 [64, 128, 256], P('gx', 'gy', 'row'), may hold values from 0.25 to 1
- weight_first: bfloat16 [512, 1024], replicated, may hold values from -0.25 to 0.25
- weight_middle: bfloat16 [1024, 1024], replicated, may hold values from -0.1875 to 0.1875
- weight_last: bfloat16 [1024, 512], replicated, may hold values from -0.1875 to 0.1875
Outputs:
- concentrations_out: float32 [2, 64, 128, 256], P(None, 'gx', 'gy', 'row')
- grad_first: float32 [512, 1024], P(('gx', 'gy', 'row'))
- grad_middle: float32 [1024, 1024], P(('gx', 'gy', 'row'))
- grad_last: float32 [1024, 512], P(('gx', 'gy', 'row'))
The draws below stay inside these ranges and needn't reach their ends.
All inputs are finite; a program needn't handle non-finite values.
Results may differ from the reference program's by a relative error of at most 0.00035.
Values may be sent and summed in bfloat16 or wider, within the bound.
No kernel may reach another device: no remote copies, remote signals or barrier semaphores. Data moves between devices by JAX's collectives and lax.ppermute only.
A program may use at most 128 MiB of HBM per device.

```python
import math
import jax
import jax.numpy as jnp
from jax import lax

STEPS = 6
PATCH = 8
HID = 1024
CELLS = 512
PATCHES_DEV = 128
NX = 64
NY = 128
NZ = 256


def steps_of(key, extent, split, least, largest):
    level, own = 1.0, jax.random.fold_in(key, 6)
    for position, parts in split:
        steps = jnp.exp(jax.random.uniform(jax.random.fold_in(own, position), (parts,), jnp.float32, least / len(split), largest / len(split)))
        level = level * jnp.repeat(steps, extent[position] // parts).reshape([-1 if axis == position else 1 for axis in range(len(extent))])
    return level


def gaussian(own_key, extent, spread, most, held_as=jnp.bfloat16):
    array = jax.random.normal(own_key, extent, jnp.float32) * spread
    return jnp.minimum(jnp.maximum(array, -most), most).astype(held_as)


def setup_inputs(seed: int = 0) -> dict:
    seeds = jax.random.split(jax.random.key(seed), 6)
    concentrations = jnp.clip(1.0 * jax.random.uniform(seeds[0], (2, NX, NY, NZ), jnp.float32) ** steps_of(seeds[0], (2, NX, NY, NZ), ((1, 4), (2, 4), (3, 2)), -0.2, 0.2), 0.0, 1.0)
    diffusivity = jnp.clip(jnp.exp(math.log(1.0) - 1.3862944 * jax.random.uniform(seeds[1], (NX, NY, NZ), jnp.float32) ** steps_of(seeds[1], (NX, NY, NZ), ((0, 4), (1, 4), (2, 2)), -0.2, 0.2)), 0.25, 1.0)
    weight_first = gaussian(seeds[2], (CELLS, HID), CELLS ** -0.5, 0.25)
    weight_middle = gaussian(seeds[3], (HID, HID), HID ** -0.5, 0.1875)
    weight_last = gaussian(seeds[4], (HID, CELLS), HID ** -0.5, 0.1875)
    return dict(concentrations=concentrations, diffusivity=diffusivity, weight_first=weight_first, weight_middle=weight_middle, weight_last=weight_last)


def laplace(values):
    summed = -6.0 * values
    for dimension in range(3):
        summed = summed + jnp.roll(values, 1, dimension) + jnp.roll(values, -1, dimension)
    return summed

def react(activator, inhibitor, diffusivity, lap_activator, lap_inhibitor, forcing):
    product = activator * inhibitor * inhibitor
    new_activator = activator + 0.1 * (diffusivity * lap_activator - product + 0.04 * (1.0 - activator) + forcing)
    new_inhibitor = inhibitor + 0.1 * (0.5 * diffusivity * lap_inhibitor + product - 0.1 * inhibitor)
    return (new_activator, new_inhibitor)

def to_patches(values, edge):
    extent_x, extent_y, extent_z = values.shape
    pieces = values.reshape(extent_x // edge, edge, extent_y // edge, edge, extent_z // edge, edge)
    return pieces.transpose(0, 2, 4, 1, 3, 5).reshape(-1, edge * edge * edge)

def from_patches(rows, shape, edge):
    extent_x, extent_y, extent_z = shape
    pieces = rows.reshape(extent_x // edge, extent_y // edge, extent_z // edge, edge, edge, edge)
    return pieces.transpose(0, 3, 1, 4, 2, 5).reshape(extent_x, extent_y, extent_z)

def gelu_back(pre_values, cotangent):
    unused, puller = jax.vjp(jax.nn.gelu, pre_values)
    return puller(cotangent)[0]

def learner(inputs, targets, weight_first, weight_middle, weight_last, scale):
    contract_rows = (((0,), (0,)), ((), ()))
    contract_cols = (((1,), (1,)), ((), ()))
    pre_first = jnp.dot(inputs, weight_first, preferred_element_type=jnp.float32)
    hidden_first = jax.nn.gelu(pre_first).astype(jnp.bfloat16)
    pre_second = jnp.dot(hidden_first, weight_middle, preferred_element_type=jnp.float32)
    hidden_second = jax.nn.gelu(pre_second).astype(jnp.bfloat16)
    forcing = jnp.dot(hidden_second, weight_last, preferred_element_type=jnp.float32)
    error = ((forcing - targets.astype(jnp.float32)) * scale).astype(jnp.bfloat16)
    grad_last = lax.dot_general(hidden_second, error, contract_rows, preferred_element_type=jnp.float32)
    carried = lax.dot_general(error, weight_last, contract_cols, preferred_element_type=jnp.float32)
    back_second = gelu_back(pre_second, carried).astype(jnp.bfloat16)
    grad_middle = lax.dot_general(hidden_first, back_second, contract_rows, preferred_element_type=jnp.float32)
    carried = lax.dot_general(back_second, weight_middle, contract_cols, preferred_element_type=jnp.float32)
    back_first = gelu_back(pre_first, carried).astype(jnp.bfloat16)
    grad_first = lax.dot_general(inputs, back_first, contract_rows, preferred_element_type=jnp.float32)
    return (forcing, grad_first, grad_middle, grad_last)

def reference(concentrations, diffusivity, weight_first, weight_middle, weight_last):
    activator = concentrations[0]
    inhibitor = concentrations[1]
    zero_force = jnp.zeros_like(activator)
    for repeat in range(STEPS // 2):
        activator, inhibitor = react(activator, inhibitor, diffusivity, laplace(activator), laplace(inhibitor), zero_force)
    inputs = to_patches(activator, PATCH).astype(jnp.bfloat16).reshape(-1, PATCHES_DEV, CELLS)
    targets = to_patches(inhibitor, PATCH).astype(jnp.bfloat16).reshape(-1, PATCHES_DEV, CELLS)
    scale = 1.0 / PATCHES_DEV

    def one_block(carry, block):
        forcing, grad_first, grad_middle, grad_last = learner(block[0], block[1], weight_first, weight_middle, weight_last, scale)
        return ((carry[0] + grad_first, carry[1] + grad_middle, carry[2] + grad_last), forcing)
    start = (jnp.zeros(weight_first.shape, jnp.float32), jnp.zeros(weight_middle.shape, jnp.float32), jnp.zeros(weight_last.shape, jnp.float32))
    grads, forcing_rows = lax.scan(one_block, start, (inputs, targets))
    forcing_field = from_patches(forcing_rows.reshape(-1, CELLS), activator.shape, PATCH)
    for repeat in range(STEPS - STEPS // 2):
        activator, inhibitor = react(activator, inhibitor, diffusivity, laplace(activator), laplace(inhibitor), forcing_field)
    return (jnp.stack([activator, inhibitor]), grads[0], grads[1], grads[2])
```

```python
import functools
import math

import jax
import jax.numpy as jnp
from jax import lax
from jax.experimental import pallas as pl
from jax.experimental.pallas import tpu as pltpu
from jax.sharding import PartitionSpec as P

STEPS = 6
PATCH = 8
VMEM_LIMIT = 48 << 20


def extended(array, sides, width):
    for axis, dim in sides:
        size, length = (lax.axis_size(axis), array.shape[dim])
        up = [(i, (i + 1) % size) for i in range(size)]
        down = [(j, i) for i, j in up]
        last = lax.slice_in_dim(array, length - width, length, axis=dim)
        leading = lax.slice_in_dim(array, 0, width, axis=dim)
        before = lax.ppermute(last, axis, up)
        after = lax.ppermute(leading, axis, down)
        array = jnp.concatenate([before, array, after], axis=dim)
    return array


def react(activator, inhibitor, diffusivity, lap_activator, lap_inhibitor, forcing):
    product = activator * inhibitor * inhibitor
    new_activator = activator + 0.1 * (
        diffusivity * lap_activator - product + 0.04 * (1.0 - activator) + forcing
    )
    new_inhibitor = inhibitor + 0.1 * (
        0.5 * diffusivity * lap_inhibitor + product - 0.1 * inhibitor
    )
    return (new_activator, new_inhibitor)


def advance(state, diffusivity, forcing):
    padded = extended(state, (("gx", 1), ("gy", 2), ("row", 3)), 1)
    center = padded[:, 1:-1, 1:-1, 1:-1]
    summed = -6.0 * center
    summed = summed + padded[:, 2:, 1:-1, 1:-1] + padded[:, :-2, 1:-1, 1:-1]
    summed = summed + padded[:, 1:-1, 2:, 1:-1] + padded[:, 1:-1, :-2, 1:-1]
    summed = summed + padded[:, 1:-1, 1:-1, 2:] + padded[:, 1:-1, 1:-1, :-2]
    new_activator, new_inhibitor = react(
        center[0], center[1], diffusivity, summed[0], summed[1], forcing
    )
    return jnp.stack([new_activator, new_inhibitor])


def to_patches(values, edge):
    extent_x, extent_y, extent_z = values.shape
    pieces = values.reshape(extent_x // edge, edge, extent_y // edge, edge, extent_z // edge, edge)
    return pieces.transpose(0, 2, 4, 1, 3, 5).reshape(-1, edge * edge * edge)


def from_patches(rows, shape, edge):
    extent_x, extent_y, extent_z = shape
    pieces = rows.reshape(extent_x // edge, extent_y // edge, extent_z // edge, edge, edge, edge)
    return pieces.transpose(0, 3, 1, 4, 2, 5).reshape(extent_x, extent_y, extent_z)


def exchange(array, mesh_sizes, flips):
    size_x, size_y, size_r = mesh_sizes
    route = []
    for i in range(size_x):
        for j in range(size_y):
            for k in range(size_r):
                here = (i * size_y + j) * size_r + k
                there = ((i ^ flips[0]) * size_y + (j ^ flips[1])) * size_r + (k ^ flips[2])
                route.append((here, there))
    return lax.ppermute(array, ("gx", "gy", "row"), route)


def reduction_stages(mesh_sizes):
    size_x, size_y, unused = mesh_sizes
    stages = []
    bit = 1
    while bit < size_x:
        stages.append((bit, 0, 0))
        bit *= 2
    bit = 2
    while bit < size_y:
        stages.append((0, bit, 0))
        bit *= 2
    return stages


def chosen_rows(total, mesh_sizes):
    size_x, size_y, size_r = mesh_sizes
    stages = reduction_stages(mesh_sizes)
    unit = total // (size_x * size_y * size_r)
    blocks = 1 << len(stages)
    position = jnp.arange(blocks * unit, dtype=jnp.int32)
    place, inner = (position // unit, position % unit)
    x = jnp.zeros_like(position) + lax.axis_index("gx")
    y = jnp.zeros_like(position) + lax.axis_index("gy")
    for number, (bit_x, bit_y, _) in enumerate(stages):
        leaves = 1 - (place >> (len(stages) - 1 - number)) % 2
        x = x ^ (leaves * bit_x)
        y = y ^ (leaves * bit_y)
    block = (x * size_y + y) * size_r + lax.axis_index("row")
    return (block * unit + inner)[:, None]


def reduce_halves(leaving, staying, mesh_sizes):
    stages = reduction_stages(mesh_sizes)
    for number, flips in enumerate(stages):
        arrived = exchange(leaving, mesh_sizes, flips)
        if number == len(stages) - 1:
            return staying + arrived
        half = staying.shape[0] // 2
        leaving = staying[:half] + arrived[:half]
        staying = staying[half:] + arrived[half:]


def gelu_pair(values):
    root = math.sqrt(2.0 / math.pi)
    square = values * values
    bend = jnp.tanh(values * (root + (root * 0.044715) * square))
    cdf = 0.5 + 0.5 * bend
    slope = cdf + (0.5 * values) * (1.0 - bend * bend) * (root + (3.0 * root * 0.044715) * square)
    return values * cdf, slope


def product(left, right):
    return jnp.dot(left, right, preferred_element_type=jnp.float32)


def product_transposed(left, right):
    return lax.dot_general(left, right, (((1,), (1,)), ((), ())), preferred_element_type=jnp.float32)


def transposed_choice(rows, source):
    columns = lax.broadcasted_iota(jnp.int32, (rows.shape[0], source.shape[1]), 1)
    choice = jnp.where(columns == rows, 1.0, 0.0).astype(jnp.bfloat16)
    return product_transposed(choice, source).astype(jnp.bfloat16)


def column_tiles(width):
    tile = 256 if width % 256 == 0 else width
    return [slice(start, start + tile) for start in range(0, width, tile)]


def store_halves(value, columns, leaving_ref, staying_ref):
    half = value.shape[0] // 2
    leaving_ref[:, columns] = value[:half]
    staying_ref[:, columns] = value[half:]


def forward_body(scale, own_ref, a_ref, b_ref, c_ref, first_ref, middle_ref, last_ref, rows_ref,
                 x_ref, h1_ref, s1_ref, h2_ref, s2_ref, error_ref, forcing_ref, leaving_ref, staying_ref):
    count = own_ref.shape[0] // 2
    parts = (own_ref, a_ref, b_ref, c_ref)
    for number, part in enumerate(parts):
        x_ref[number * count:(number + 1) * count, :] = part[:count, :]
    x = x_ref[...]
    for columns in column_tiles(h1_ref.shape[1]):
        value, slope = gelu_pair(product(x, first_ref[:, columns]))
        h1_ref[:, columns] = value.astype(jnp.bfloat16)
        s1_ref[:, columns] = slope
    h1 = h1_ref[...]
    for columns in column_tiles(h2_ref.shape[1]):
        value, slope = gelu_pair(product(h1, middle_ref[:, columns]))
        h2_ref[:, columns] = value.astype(jnp.bfloat16)
        s2_ref[:, columns] = slope
    h2 = h2_ref[...]
    for columns in column_tiles(error_ref.shape[1]):
        forcing = product(h2, last_ref[:, columns])
        forcing_ref[:, columns] = forcing[:count]
        for number, part in enumerate(parts):
            block = slice(number * count, (number + 1) * count)
            target = part[count:, columns].astype(jnp.float32)
            error_ref[block, columns] = ((forcing[block] - target) * scale).astype(jnp.bfloat16)
    chosen = transposed_choice(rows_ref[...], h2)
    for columns in column_tiles(error_ref.shape[1]):
        store_halves(product(chosen, error_ref[:, columns]), columns, leaving_ref, staying_ref)


def backward_body(carried_ref, weight_ref, slope_ref, source_ref, rows_ref, back_ref, leaving_ref, staying_ref):
    carried = carried_ref[...]
    for columns in column_tiles(back_ref.shape[1]):
        value = product_transposed(carried, weight_ref[columns, :]) * slope_ref[:, columns]
        back_ref[:, columns] = value.astype(jnp.bfloat16)
    chosen = transposed_choice(rows_ref[...], source_ref[...])
    for columns in column_tiles(back_ref.shape[1]):
        store_halves(product(chosen, back_ref[:, columns]), columns, leaving_ref, staying_ref)


def kernel_call(body, outputs, name):
    return pl.pallas_call(
        body,
        out_shape=[jax.ShapeDtypeStruct(shape, dtype) for shape, dtype in outputs],
        compiler_params=pltpu.CompilerParams(vmem_limit_bytes=VMEM_LIMIT),
        name=name,
    )


def learner(own, mesh_sizes, weight_first, weight_middle, weight_last):
    f32, bf16 = (jnp.float32, jnp.bfloat16)
    count = own.shape[0] // 2
    cells, hidden = weight_first.shape
    hidden_second = weight_middle.shape[1]
    others = [exchange(own, mesh_sizes, flips) for flips in ((0, 0, 1), (0, 1, 0), (0, 1, 1))]
    total = 4 * count
    rows_first, rows_middle, rows_last = [chosen_rows(size, mesh_sizes) for size in (cells, hidden, hidden_second)]
    part = lambda rows, width: ((rows.shape[0] // 2, width), f32)
    x, h1, s1, h2, s2, error, forcing, *last = kernel_call(
        functools.partial(forward_body, 1.0 / count),
        [((total, cells), bf16), ((total, hidden), bf16), ((total, hidden), f32), ((total, hidden_second), bf16),
         ((total, hidden_second), f32), ((total, cells), bf16), ((count, cells), f32),
         part(rows_last, cells), part(rows_last, cells)],
        "forward",
    )(own, *others, weight_first, weight_middle, weight_last, rows_last)
    back_second, *middle = kernel_call(
        backward_body,
        [((total, hidden_second), bf16), part(rows_middle, hidden_second), part(rows_middle, hidden_second)],
        "backward_second",
    )(error, weight_last, s2, h1, rows_middle)
    back_first, *first = kernel_call(
        backward_body,
        [((total, hidden), bf16), part(rows_first, hidden), part(rows_first, hidden)],
        "backward_first",
    )(back_second, weight_middle, s1, x, rows_first)
    return forcing, [reduce_halves(*pair, mesh_sizes) for pair in (first, middle, last)]


def per_device(concentrations, diffusivity, weight_first, weight_middle, weight_last):
    mesh_sizes = tuple(lax.axis_size(axis) for axis in ("gx", "gy", "row"))
    state = concentrations
    zero_force = jnp.zeros(state.shape[1:], jnp.float32)
    for repeat in range(STEPS // 2):
        state = advance(state, diffusivity, zero_force)
    inputs = to_patches(state[0], PATCH).astype(jnp.bfloat16)
    targets = to_patches(state[1], PATCH).astype(jnp.bfloat16)
    own = jnp.concatenate([inputs, targets])
    forcing_rows, grads = learner(own, mesh_sizes, weight_first, weight_middle, weight_last)
    forcing_field = from_patches(forcing_rows, state.shape[1:], PATCH)
    for repeat in range(STEPS - STEPS // 2):
        state = advance(state, diffusivity, forcing_field)
    return (state, *grads)


def solution(mesh):
    in_specs = (P(None, "gx", "gy", "row"), P("gx", "gy", "row"), P(), P(), P())
    out_specs = (
        P(None, "gx", "gy", "row"),
        P(("gx", "gy", "row"), None),
        P(("gx", "gy", "row"), None),
        P(("gx", "gy", "row"), None),
    )
    return jax.shard_map(
        per_device, mesh=mesh, in_specs=in_specs, out_specs=out_specs, check_vma=False
    )
```

```python
import functools
import math

import jax
import jax.numpy as jnp
from jax import lax
from jax.experimental import pallas as pl
from jax.experimental.pallas import tpu as pltpu
from jax.sharding import PartitionSpec as P

STEPS = 6
PATCH = 8
HALO = STEPS // 2
EDGE = 4
VMEM_LIMIT = 48 << 20


def ring(array, axis, distance):
    size = lax.axis_size(axis)
    return lax.ppermute(array, axis, [(i, (i + distance) % size) for i in range(size)])


def react(activator, inhibitor, diffusivity, lap_activator, lap_inhibitor, forcing):
    product = activator * inhibitor * inhibitor
    inner = diffusivity * lap_activator - product + 0.04 * (1.0 - activator)
    new_activator = activator + 0.1 * (inner if forcing is None else inner + forcing)
    new_inhibitor = inhibitor + 0.1 * (
        0.5 * diffusivity * lap_inhibitor + product - 0.1 * inhibitor
    )
    return (new_activator, new_inhibitor)


def fields(state, third):
    return ((lambda x, rows: state[0, x, rows, :], HALO), (lambda x, rows: state[1, x, rows, :], HALO),
            (lambda x, rows: third[x, rows, :], HALO - 1))


def plane_of(state, third, before, after, kind, plane, rows):
    read, depth = fields(state, third)[kind]
    length = state.shape[1]
    x = plane - HALO
    if x < -depth or x >= length + depth:
        return None
    if x < 0:
        return before[kind * HALO + depth + x, rows, :]
    if x >= length:
        return after[kind * HALO + x - length, rows, :]
    return read(x, rows)


def edge_rows_body(state, third, before, after, leading_ref, trailing_ref):
    length, height = state.shape[1:3]
    for plane in range(length + 2 * HALO):
        for kind, depth in enumerate((HALO, HALO, HALO - 1)):
            for out_ref, start in ((leading_ref, 0), (trailing_ref, height - depth)):
                value = plane_of(state, third, before, after, kind, plane, slice(start, start + depth))
                if value is None:
                    value = jnp.zeros((depth, state.shape[3]), jnp.float32)
                out_ref[plane, kind * HALO:kind * HALO + depth, :] = value


def strips_of(planes, width):
    each = width // (2 * HALO)
    places = {}
    for kind in range(3):
        for plane in range(kind // 2, planes - kind // 2):
            number = len(places)
            places[kind, plane] = (number // each, (number % each) * 2 * HALO)
    return places, -(-len(places) // each)


def assemble_body(state, third, before, after, below, above, whole_ref, strips_ref):
    length, height, width = state.shape[1:]
    planes = length + 2 * HALO
    places, unused = strips_of(planes, width)
    lanes = lax.broadcasted_iota(jnp.int32, whole_ref.shape[2:], 1)
    tiles = {}
    for kind, depth in enumerate((HALO, HALO, HALO - 1)):
        for plane in range(planes):
            value = plane_of(state, third, before, after, kind, plane, slice(0, height))
            if value is None:
                continue
            held = slice(kind * HALO, kind * HALO + depth)
            whole_ref[kind, plane, EDGE:EDGE + height, :] = value
            whole_ref[kind, plane, EDGE - depth:EDGE, :] = below[plane, held, :]
            whole_ref[kind, plane, EDGE + height:EDGE + height + depth, :] = above[plane, held, :]
            tile, shift = places[kind, plane]
            turned = pltpu.roll(whole_ref[kind, plane], (shift + HALO) % width, axis=1)
            here = (lanes >= shift) & (lanes < shift + 2 * HALO)
            tiles[tile] = jnp.where(here, turned, tiles[tile]) if tile in tiles else turned
    for tile, value in tiles.items():
        strips_ref[tile] = value


def load_wide(whole, earlier, later, kind, target, places):
    rows, width = whole.shape[2:]
    lanes = lax.broadcasted_iota(jnp.int32, (rows, width), 1)
    for plane in range(whole.shape[1]):
        if (kind, plane) not in places:
            continue
        tile, shift = places[kind, plane]
        back = (2 * width - shift - HALO) % width
        beside = later[tile] if later is earlier else jnp.where(
            (lanes >= shift + HALO) & (lanes < shift + 2 * HALO), later[tile], earlier[tile])
        target[plane, 8:8 + rows, :width] = whole[kind, plane]
        target[plane, 8:8 + rows, width:] = pltpu.roll(beside, back, axis=1)


def one_step(source, target, diffusivity, forcing, planes, rows):
    first, last = rows

    def one_plane(plane, carry):
        laps = []
        for field in source:
            center = field[plane, first:last, :]
            width = center.shape[1]
            summed = -6.0 * center + field[plane + 1, first:last, :] + field[plane - 1, first:last, :]
            summed = summed + field[plane, first + 1:last + 1, :] + field[plane, first - 1:last - 1, :]
            laps.append(summed + pltpu.roll(center, 1, axis=1) + pltpu.roll(center, width - 1, axis=1))
        extra = None if forcing is None else forcing[plane, first:last, :]
        new = react(source[0][plane, first:last, :], source[1][plane, first:last, :],
                    diffusivity[plane, first:last, :], *laps, extra)
        for field, value in zip(target, new):
            field[plane, first:last, :] = value
        return carry

    lax.fori_loop(planes[0], planes[1], one_plane, 0)


def run_steps(now, then, diffusivity, forcing, rows):
    planes = now[0].shape[0]
    for step in range(HALO):
        one_step(now, then, diffusivity, forcing, (step + 1, planes - step - 1), (8, 8 + rows))
        now, then = then, now
    return now


def move_order(patches_z, edge):
    lanes = patches_z * edge
    row = lax.broadcasted_iota(jnp.int32, (lanes, lanes), 0)
    column = lax.broadcasted_iota(jnp.int32, (lanes, lanes), 1)
    return jnp.where((row % patches_z) * edge + row // patches_z == column, 1.0, 0.0).astype(jnp.bfloat16)


def cell_order(edge):
    cells = edge ** 3
    row = lax.broadcasted_iota(jnp.int32, (cells, cells), 0)
    column = lax.broadcasted_iota(jnp.int32, (cells, cells), 1)
    return jnp.where((row % (edge * edge)) * edge + row // (edge * edge) == column, 1.0, 0.0).astype(jnp.bfloat16)


def half_tiles(source, count, rows, by_lane):
    half = by_lane // 2
    lanes = lax.broadcasted_iota(jnp.int32, (rows, by_lane), 1)
    out = []
    for b in range(count[1]):
        tiles = []
        for a in range(0, count[0], 2):
            low, high = [source[n * rows:(n + 1) * rows, (b // 2) * by_lane:(b // 2 + 1) * by_lane] for n in (a, a + 1)]
            if b % 2 == 0:
                high = pltpu.roll(high, half, axis=1)
            else:
                low = pltpu.roll(low, half, axis=1)
            tiles.append(jnp.where(lanes < half, low, high))
        out.append(jnp.concatenate(tiles, axis=1))
    return jnp.concatenate(out, axis=0)


def cube_starts(shape, edge):
    extent_x, extent_y = shape
    return [(px * edge + ix, py * edge) for px in range(extent_x // edge) for py in range(extent_y // edge)
            for ix in range(edge)]


def exact_product(left, right):
    high = left.astype(jnp.bfloat16)
    low = (left - high.astype(jnp.float32)).astype(jnp.bfloat16)
    return product(high, right) + product(low, right)


def first_steps_body(edge, whole, earlier, later, state_ref, own_ref, wide_ref, u0, v0, u1, v1, column_ref):
    length, height, width = state_ref.shape[1:]
    places, unused = strips_of(whole.shape[1], width)
    wide = wide_ref
    for kind, target in enumerate((u0, v0, wide)):
        load_wide(whole, earlier, later, kind, target, places)
    now = run_steps((u0, v0), (u1, v1), wide, None, whole.shape[2])
    move, order = (move_order(width // edge, edge), cell_order(edge))
    count = own_ref.shape[0] // 2
    for species, field in enumerate(now):
        for x in range(length):
            state_ref[species, x] = field[x + HALO, 8 + EDGE:8 + EDGE + height, :width]
        for number, (x, y) in enumerate(cube_starts((length, height), edge)):
            column_ref[number * edge:(number + 1) * edge, :] = state_ref[species, x, y:y + edge, :]
        turned = product_transposed(move, column_ref[...].astype(jnp.bfloat16))
        columns = length * height // (edge * edge)
        cubes = half_tiles(turned, (edge, columns), width // edge, 2 * edge * edge)
        own_ref[species * count:(species + 1) * count, :] = product(cubes.astype(jnp.bfloat16), order).astype(jnp.bfloat16)


def own_forward_body(edge, own_ref, first_ref, middle_ref, last_ref, field_ref):
    length, height, width = field_ref.shape
    count = own_ref.shape[0] // 2
    h1 = gelu_value(product(own_ref[:count, :], first_ref[...])).astype(jnp.bfloat16)
    h2 = gelu_value(product(h1, middle_ref[...])).astype(jnp.bfloat16)
    forcing = product(h2, last_ref[...])
    cells = lax.broadcasted_iota(jnp.int32, (edge ** 3, edge ** 3), 1)
    row = lax.broadcasted_iota(jnp.int32, (edge ** 3, edge ** 3), 0)
    square = edge * edge
    order = jnp.where((cells % square) * edge + cells // square == row, 1.0, 0.0).astype(jnp.bfloat16)
    columns = length * height // square
    turned = half_tiles(exact_product(forcing, order), (columns, edge), width // edge, 2 * square)
    moved = exact_product(turned.T, move_order(width // edge, edge))
    for number, (x, y) in enumerate(cube_starts((length, height), edge)):
        field_ref[x, y:y + edge, :] = moved[number * edge:(number + 1) * edge, :]


def last_steps_body(whole, earlier, later, wide, state_ref, u0, v0, u1, v1, force):
    length, height, width = state_ref.shape[1:]
    places, unused = strips_of(whole.shape[1], width)
    for kind, target in enumerate((u0, v0, force)):
        load_wide(whole, earlier, later, kind, target, places)
    now = run_steps((u0, v0), (u1, v1), wide, force, whole.shape[2])
    for species, field in enumerate(now):
        for x in range(length):
            state_ref[species, x] = field[x + HALO, 8 + EDGE:8 + EDGE + height, :width]


def with_halos(state, third, name):
    length, height, width = state.shape[1:]
    planes = length + 2 * HALO
    f32 = jnp.float32
    leading = jnp.concatenate([state[0, :HALO], state[1, :HALO], third[:HALO - 1]])
    trailing = jnp.concatenate([state[0, -HALO:], state[1, -HALO:], third[1 - HALO:]])
    before, after = (ring(trailing, "gx", 1), ring(leading, "gx", -1))
    leading, trailing = kernel_call(
        edge_rows_body, [((planes, 3 * HALO - 1, width), f32)] * 2, name + "_rows"
    )(state, third, before, after)
    below, above = (ring(trailing, "gy", 1), ring(leading, "gy", -1))
    whole, strips = kernel_call(
        assemble_body,
        [((3, planes, height + 2 * EDGE, width), f32), ((strips_of(planes, width)[1], height + 2 * EDGE, width), f32)],
        name + "_assemble",
    )(state, third, before, after, below, above)
    earlier = ring(strips, "row", 1)
    later = earlier if lax.axis_size("row") == 2 else ring(strips, "row", -1)
    return whole, earlier, later


def exchange(array, mesh_sizes, flips):
    size_x, size_y, size_r = mesh_sizes
    route = []
    for i in range(size_x):
        for j in range(size_y):
            for k in range(size_r):
                here = (i * size_y + j) * size_r + k
                there = ((i ^ flips[0]) * size_y + (j ^ flips[1])) * size_r + (k ^ flips[2])
                route.append((here, there))
    return lax.ppermute(array, ("gx", "gy", "row"), route)


def reduction_stages(mesh_sizes):
    size_x, size_y, unused = mesh_sizes
    stages = []
    bit = 1
    while bit < size_x:
        stages.append((bit, 0, 0))
        bit *= 2
    bit = 2
    while bit < size_y:
        stages.append((0, bit, 0))
        bit *= 2
    return stages


def chosen_rows(total, mesh_sizes):
    size_x, size_y, size_r = mesh_sizes
    stages = reduction_stages(mesh_sizes)
    unit = total // (size_x * size_y * size_r)
    blocks = 1 << len(stages)
    position = jnp.arange(blocks * unit, dtype=jnp.int32)
    place, inner = (position // unit, position % unit)
    x = jnp.zeros_like(position) + lax.axis_index("gx")
    y = jnp.zeros_like(position) + lax.axis_index("gy")
    for number, (bit_x, bit_y, _) in enumerate(stages):
        leaves = 1 - (place >> (len(stages) - 1 - number)) % 2
        x = x ^ (leaves * bit_x)
        y = y ^ (leaves * bit_y)
    block = (x * size_y + y) * size_r + lax.axis_index("row")
    return (block * unit + inner)[:, None]


def reduce_halves(leaving, staying, mesh_sizes):
    stages = reduction_stages(mesh_sizes)
    for number, flips in enumerate(stages):
        arrived = exchange(leaving, mesh_sizes, flips)
        if number == len(stages) - 1:
            return staying + arrived
        half = staying.shape[0] // 2
        leaving = staying[:half] + arrived[:half]
        staying = staying[half:] + arrived[half:]


def gelu_pair(values):
    root = math.sqrt(2.0 / math.pi)
    square = values * values
    bend = jnp.tanh(values * (root + (root * 0.044715) * square))
    cdf = 0.5 + 0.5 * bend
    slope = cdf + (0.5 * values) * (1.0 - bend * bend) * (root + (3.0 * root * 0.044715) * square)
    return values * cdf, slope


def gelu_value(values):
    root = math.sqrt(2.0 / math.pi)
    return values * (0.5 + 0.5 * jnp.tanh(values * (root + (root * 0.044715) * (values * values))))


def product(left, right):
    return jnp.dot(left, right, preferred_element_type=jnp.float32)


def product_transposed(left, right):
    return lax.dot_general(left, right, (((1,), (1,)), ((), ())), preferred_element_type=jnp.float32)


def transposed_choice(rows, source):
    columns = lax.broadcasted_iota(jnp.int32, (rows.shape[0], source.shape[1]), 1)
    choice = jnp.where(columns == rows, 1.0, 0.0).astype(jnp.bfloat16)
    return product_transposed(choice, source).astype(jnp.bfloat16)


def column_tiles(width):
    tile = 256 if width % 256 == 0 else width
    return [slice(start, start + tile) for start in range(0, width, tile)]


def store_halves(value, columns, leaving_ref, staying_ref):
    half = value.shape[0] // 2
    leaving_ref[:, columns] = value[:half]
    staying_ref[:, columns] = value[half:]


def forward_body(scale, own_ref, a_ref, b_ref, c_ref, first_ref, middle_ref, last_ref, rows_ref,
                 x_ref, h1_ref, s1_ref, h2_ref, s2_ref, error_ref, leaving_ref, staying_ref):
    count = own_ref.shape[0] // 2
    parts = (own_ref, a_ref, b_ref, c_ref)
    for number, part in enumerate(parts):
        x_ref[number * count:(number + 1) * count, :] = part[:count, :]
    x = x_ref[...]
    for columns in column_tiles(h1_ref.shape[1]):
        value, slope = gelu_pair(product(x, first_ref[:, columns]))
        h1_ref[:, columns] = value.astype(jnp.bfloat16)
        s1_ref[:, columns] = slope
    h1 = h1_ref[...]
    for columns in column_tiles(h2_ref.shape[1]):
        value, slope = gelu_pair(product(h1, middle_ref[:, columns]))
        h2_ref[:, columns] = value.astype(jnp.bfloat16)
        s2_ref[:, columns] = slope
    h2 = h2_ref[...]
    for columns in column_tiles(error_ref.shape[1]):
        forcing = product(h2, last_ref[:, columns])
        for number, part in enumerate(parts):
            block = slice(number * count, (number + 1) * count)
            target = part[count:, columns].astype(jnp.float32)
            error_ref[block, columns] = ((forcing[block] - target) * scale).astype(jnp.bfloat16)
    chosen = transposed_choice(rows_ref[...], h2)
    for columns in column_tiles(error_ref.shape[1]):
        store_halves(product(chosen, error_ref[:, columns]), columns, leaving_ref, staying_ref)


def backward_body(carried_ref, weight_ref, slope_ref, source_ref, rows_ref, back_ref, leaving_ref, staying_ref):
    carried = carried_ref[...]
    for columns in column_tiles(back_ref.shape[1]):
        value = product_transposed(carried, weight_ref[columns, :]) * slope_ref[:, columns]
        back_ref[:, columns] = value.astype(jnp.bfloat16)
    chosen = transposed_choice(rows_ref[...], source_ref[...])
    for columns in column_tiles(back_ref.shape[1]):
        store_halves(product(chosen, back_ref[:, columns]), columns, leaving_ref, staying_ref)


def kernel_call(body, outputs, name, scratch=()):
    return pl.pallas_call(
        body,
        out_shape=[jax.ShapeDtypeStruct(shape, dtype) for shape, dtype in outputs],
        scratch_shapes=[pltpu.VMEM(shape, dtype) for shape, dtype in scratch],
        compiler_params=pltpu.CompilerParams(vmem_limit_bytes=VMEM_LIMIT),
        name=name,
    )


def learner(own, others, mesh_sizes, weight_first, weight_middle, weight_last):
    f32, bf16 = (jnp.float32, jnp.bfloat16)
    count = own.shape[0] // 2
    cells, hidden = weight_first.shape
    hidden_second = weight_middle.shape[1]
    total = 4 * count
    rows_first, rows_middle, rows_last = [chosen_rows(size, mesh_sizes) for size in (cells, hidden, hidden_second)]
    part = lambda rows, width: ((rows.shape[0] // 2, width), f32)
    x, h1, s1, h2, s2, error, *last = kernel_call(
        functools.partial(forward_body, 1.0 / count),
        [((total, cells), bf16), ((total, hidden), bf16), ((total, hidden), f32), ((total, hidden_second), bf16),
         ((total, hidden_second), f32), ((total, cells), bf16),
         part(rows_last, cells), part(rows_last, cells)],
        "forward",
    )(own, *others, weight_first, weight_middle, weight_last, rows_last)
    back_second, *middle = kernel_call(
        backward_body,
        [((total, hidden_second), bf16), part(rows_middle, hidden_second), part(rows_middle, hidden_second)],
        "backward_second",
    )(error, weight_last, s2, h1, rows_middle)
    back_first, *first = kernel_call(
        backward_body,
        [((total, hidden), bf16), part(rows_first, hidden), part(rows_first, hidden)],
        "backward_first",
    )(back_second, weight_middle, s1, x, rows_first)
    return [reduce_halves(*pair, mesh_sizes) for pair in (first, middle, last)]


def per_device(concentrations, diffusivity, weight_first, weight_middle, weight_last):
    mesh_sizes = tuple(lax.axis_size(axis) for axis in ("gx", "gy", "row"))
    length, height, width = diffusivity.shape
    f32 = jnp.float32
    planes, rows = (length + 2 * HALO, height + 2 * EDGE)
    wide = ((planes, 8 + rows + 8, 2 * width), f32)
    count = length * height * width // PATCH ** 3
    weights = (weight_first, weight_middle, weight_last)
    state, own, wide_diffusivity = kernel_call(
        functools.partial(first_steps_body, PATCH),
        [(concentrations.shape, f32), ((2 * count, PATCH ** 3), jnp.bfloat16), wide],
        "first_steps",
        scratch=[wide] * 4 + [((length * height, width), f32)],
    )(*with_halos(concentrations, diffusivity, "first"))
    others = [exchange(own, mesh_sizes, flips) for flips in ((0, 0, 1), (0, 1, 0), (0, 1, 1))]
    (field,) = kernel_call(functools.partial(own_forward_body, PATCH), [(diffusivity.shape, f32)], "own_forward")(
        own, *weights
    )
    grads = learner(own, others, mesh_sizes, *weights)
    (state,) = kernel_call(last_steps_body, [(state.shape, f32)], "last_steps", scratch=[wide] * 5)(
        *with_halos(state, field, "last"), wide_diffusivity
    )
    return (state, *grads)


def solution(mesh):
    in_specs = (P(None, "gx", "gy", "row"), P("gx", "gy", "row"), P(), P(), P())
    out_specs = (
        P(None, "gx", "gy", "row"),
        P(("gx", "gy", "row"), None),
        P(("gx", "gy", "row"), None),
        P(("gx", "gy", "row"), None),
    )
    return jax.shard_map(
        per_device, mesh=mesh, in_specs=in_specs, out_specs=out_specs, check_vma=False
    )
```

```python
import functools
import math

import jax
import jax.numpy as jnp
from jax import lax
from jax.experimental import pallas as pl
from jax.experimental.pallas import tpu as pltpu
from jax.sharding import PartitionSpec as P

STEPS = 6
PATCH = 8
HALO = STEPS // 2
EDGE = 4
VMEM_LIMIT = 20 << 20


def ring(array, axis, distance):
    size = lax.axis_size(axis)
    return lax.ppermute(array, axis, [(i, (i + distance) % size) for i in range(size)])


def react(activator, inhibitor, diffusivity, lap_activator, lap_inhibitor, forcing):
    product = activator * inhibitor * inhibitor
    inner = diffusivity * lap_activator - product + 0.04 * (1.0 - activator)
    new_activator = activator + 0.1 * (inner if forcing is None else inner + forcing)
    new_inhibitor = inhibitor + 0.1 * (
        0.5 * diffusivity * lap_inhibitor + product - 0.1 * inhibitor
    )
    return (new_activator, new_inhibitor)


def fields(state, third):
    return ((lambda x, rows: state[0, x, rows, :], HALO), (lambda x, rows: state[1, x, rows, :], HALO),
            (lambda x, rows: third[x, rows, :], HALO - 1))


def plane_of(state, third, before, after, kind, plane, rows):
    read, depth = fields(state, third)[kind]
    length = state.shape[1]
    x = plane - HALO
    if x < -depth or x >= length + depth:
        return None
    if x < 0:
        return before[kind * HALO + depth + x, rows, :]
    if x >= length:
        return after[kind * HALO + x - length, rows, :]
    return read(x, rows)


def edge_rows_body(state, third, before, after, leading_ref, trailing_ref):
    length, height = state.shape[1:3]
    for plane in range(length + 2 * HALO):
        for kind, depth in enumerate((HALO, HALO, HALO - 1)):
            for out_ref, start in ((leading_ref, 0), (trailing_ref, height - depth)):
                value = plane_of(state, third, before, after, kind, plane, slice(start, start + depth))
                if value is None:
                    value = jnp.zeros((depth, state.shape[3]), jnp.float32)
                out_ref[plane, kind * HALO:kind * HALO + depth, :] = value


def strips_of(planes, width):
    each = width // (2 * HALO)
    places = {}
    for kind in range(3):
        for plane in range(kind // 2, planes - kind // 2):
            number = len(places)
            places[kind, plane] = (number // each, (number % each) * 2 * HALO)
    return places, -(-len(places) // each)


def assemble_body(state, third, before, after, below, above, whole_ref, strips_ref):
    length, height, width = state.shape[1:]
    planes = length + 2 * HALO
    places, _ = strips_of(planes, width)
    lanes = lax.broadcasted_iota(jnp.int32, whole_ref.shape[2:], 1)
    tiles = {}
    for kind, depth in enumerate((HALO, HALO, HALO - 1)):
        for plane in range(planes):
            value = plane_of(state, third, before, after, kind, plane, slice(0, height))
            if value is None:
                continue
            held = slice(kind * HALO, kind * HALO + depth)
            whole_ref[kind, plane, EDGE:EDGE + height, :] = value
            whole_ref[kind, plane, EDGE - depth:EDGE, :] = below[plane, held, :]
            whole_ref[kind, plane, EDGE + height:EDGE + height + depth, :] = above[plane, held, :]
            tile, shift = places[kind, plane]
            turned = pltpu.roll(whole_ref[kind, plane], (shift + HALO) % width, axis=1)
            here = (lanes >= shift) & (lanes < shift + 2 * HALO)
            tiles[tile] = jnp.where(here, turned, tiles[tile]) if tile in tiles else turned
    for tile, value in tiles.items():
        strips_ref[tile] = value


def load_wide(whole, earlier, later, kind, target, places):
    rows, width = whole.shape[2:]
    lanes = lax.broadcasted_iota(jnp.int32, (rows, width), 1)
    for plane in range(whole.shape[1]):
        if (kind, plane) not in places:
            continue
        tile, shift = places[kind, plane]
        back = (2 * width - shift - HALO) % width
        beside = later[tile] if later is earlier else jnp.where(
            (lanes >= shift + HALO) & (lanes < shift + 2 * HALO), later[tile], earlier[tile])
        target[plane, 8:8 + rows, :width] = whole[kind, plane]
        target[plane, 8:8 + rows, width:] = pltpu.roll(beside, back, axis=1)


def one_step(source, target, diffusivity, forcing, planes, rows):
    first, last = rows

    def one_plane(plane, carry):
        laps = []
        for field in source:
            center = field[plane, first:last, :]
            width = center.shape[1]
            summed = -6.0 * center + field[plane + 1, first:last, :] + field[plane - 1, first:last, :]
            summed = summed + field[plane, first + 1:last + 1, :] + field[plane, first - 1:last - 1, :]
            laps.append(summed + pltpu.roll(center, 1, axis=1) + pltpu.roll(center, width - 1, axis=1))
        extra = None if forcing is None else forcing[plane, first:last, :]
        new = react(source[0][plane, first:last, :], source[1][plane, first:last, :],
                    diffusivity[plane, first:last, :], *laps, extra)
        for field, value in zip(target, new):
            field[plane, first:last, :] = value
        return carry

    lax.fori_loop(planes[0], planes[1], one_plane, 0)


def run_steps(now, then, diffusivity, forcing, rows):
    planes = now[0].shape[0]
    for step in range(HALO):
        one_step(now, then, diffusivity, forcing, (step + 1, planes - step - 1), (8, 8 + rows))
        now, then = then, now
    return now


def move_order(patches_z, edge):
    lanes = patches_z * edge
    row = lax.broadcasted_iota(jnp.int32, (lanes, lanes), 0)
    column = lax.broadcasted_iota(jnp.int32, (lanes, lanes), 1)
    return jnp.where((row % patches_z) * edge + row // patches_z == column, 1.0, 0.0).astype(jnp.bfloat16)


def cell_order(edge):
    cells = edge ** 3
    row = lax.broadcasted_iota(jnp.int32, (cells, cells), 0)
    column = lax.broadcasted_iota(jnp.int32, (cells, cells), 1)
    return jnp.where((row % (edge * edge)) * edge + row // (edge * edge) == column, 1.0, 0.0).astype(jnp.bfloat16)


def half_tiles(source, count, rows, by_lane):
    half = by_lane // 2
    lanes = lax.broadcasted_iota(jnp.int32, (rows, by_lane), 1)
    out = []
    for b in range(count[1]):
        tiles = []
        for a in range(0, count[0], 2):
            low, high = [source[n * rows:(n + 1) * rows, (b // 2) * by_lane:(b // 2 + 1) * by_lane] for n in (a, a + 1)]
            if b % 2 == 0:
                high = pltpu.roll(high, half, axis=1)
            else:
                low = pltpu.roll(low, half, axis=1)
            tiles.append(jnp.where(lanes < half, low, high))
        out.append(jnp.concatenate(tiles, axis=1))
    return jnp.concatenate(out, axis=0)


def cube_starts(shape, edge):
    extent_x, extent_y = shape
    return [(px * edge + ix, py * edge) for px in range(extent_x // edge) for py in range(extent_y // edge)
            for ix in range(edge)]


def exact_product(left, right):
    high = left.astype(jnp.bfloat16)
    low = (left - high.astype(jnp.float32)).astype(jnp.bfloat16)
    return product(high, right) + product(low, right)


def first_steps_body(edge, whole, earlier, later, state_ref, own_ref, wide_ref, u0, v0, u1, v1, wide, column_ref, semaphores):
    length, height, width = state_ref.shape[1:]
    places, _ = strips_of(whole.shape[1], width)
    for kind, target in enumerate((u0, v0, wide)):
        load_wide(whole, earlier, later, kind, target, places)
    (copy,) = start_copies([(wide, wide_ref)], semaphores)
    now = run_steps((u0, v0), (u1, v1), wide, None, whole.shape[2])
    move, order = (move_order(width // edge, edge), cell_order(edge))
    count = own_ref.shape[0] // 2
    for species, field in enumerate(now):
        for x in range(length):
            state_ref[species, x] = field[x + HALO, 8 + EDGE:8 + EDGE + height, :width]
        for number, (x, y) in enumerate(cube_starts((length, height), edge)):
            column_ref[number * edge:(number + 1) * edge, :] = state_ref[species, x, y:y + edge, :]
        turned = product_transposed(move, column_ref[...].astype(jnp.bfloat16))
        columns = length * height // (edge * edge)
        cubes = half_tiles(turned, (edge, columns), width // edge, 2 * edge * edge)
        own_ref[species * count:(species + 1) * count, :] = product(cubes.astype(jnp.bfloat16), order).astype(jnp.bfloat16)
    copy.wait()


def own_forward_body(edge, own_ref, first_ref, middle_ref, last_ref, field_ref):
    length, height, width = field_ref.shape
    count = own_ref.shape[0] // 2
    h1 = gelu_value(product(own_ref[:count, :], first_ref[...])).astype(jnp.bfloat16)
    h2 = gelu_value(product(h1, middle_ref[...])).astype(jnp.bfloat16)
    forcing = product(h2, last_ref[...])
    cells = lax.broadcasted_iota(jnp.int32, (edge ** 3, edge ** 3), 1)
    row = lax.broadcasted_iota(jnp.int32, (edge ** 3, edge ** 3), 0)
    square = edge * edge
    order = jnp.where((cells % square) * edge + cells // square == row, 1.0, 0.0).astype(jnp.bfloat16)
    columns = length * height // square
    turned = half_tiles(exact_product(forcing, order), (columns, edge), width // edge, 2 * square)
    moved = exact_product(turned.T, move_order(width // edge, edge))
    for number, (x, y) in enumerate(cube_starts((length, height), edge)):
        field_ref[x, y:y + edge, :] = moved[number * edge:(number + 1) * edge, :]


def last_steps_body(whole, earlier, later, wide, state_ref, u0, v0, u1, v1, force):
    length, height, width = state_ref.shape[1:]
    places, _ = strips_of(whole.shape[1], width)
    for kind, target in enumerate((u0, v0, force)):
        load_wide(whole, earlier, later, kind, target, places)
    now = run_steps((u0, v0), (u1, v1), wide, force, whole.shape[2])
    for species, field in enumerate(now):
        for x in range(length):
            state_ref[species, x] = field[x + HALO, 8 + EDGE:8 + EDGE + height, :width]


def start_copies(pairs, semaphores):
    copies = [pltpu.make_async_copy(*pair, semaphores.at[number]) for number, pair in enumerate(pairs)]
    for copy in copies:
        copy.start()
    return copies


def store_faces(state, third, leading_ref, trailing_ref):
    length = third.shape[0]
    for kind, depth in enumerate((HALO, HALO, HALO - 1)):
        read = fields(state, third)[kind][0]
        for plane in range(depth):
            leading_ref[kind * HALO + plane] = read(plane, slice(None))
            trailing_ref[kind * HALO + plane] = read(length - depth + plane, slice(None))


def first_faces_body(state_ref, third_ref, leading_ref, trailing_ref, state_out, third_out, semaphores):
    for copy in start_copies(((state_ref, state_out), (third_ref, third_out)), semaphores):
        copy.wait()
    store_faces(state_out, third_out, leading_ref, trailing_ref)


def x_halos(leading, trailing):
    return ring(trailing, "gx", 1), ring(leading, "gx", -1)


def edge_rows(state, third, before, after):
    planes = state.shape[1] + 2 * HALO
    return kernel_call(edge_rows_body, [((planes, 3 * HALO - 1, state.shape[3]), jnp.float32)] * 2)(
        state, third, before, after
    )


def y_halos(leading, trailing):
    return ring(trailing, "gy", 1), ring(leading, "gy", -1)


def assemble(state, third, before, after, below, above):
    length, height, width = state.shape[1:]
    planes, rows = (length + 2 * HALO, height + 2 * EDGE)
    outputs = [(3, planes, rows, width), (strips_of(planes, width)[1], rows, width)]
    return kernel_call(assemble_body, [(shape, jnp.float32) for shape in outputs])(
        state, third, before, after, below, above
    )


def z_strips(strips):
    earlier = ring(strips, "row", 1)
    return earlier, (earlier if lax.axis_size("row") == 2 else ring(strips, "row", -1))


def exchange(array, mesh_sizes, flips):
    size_x, size_y, size_r = mesh_sizes
    route = []
    for i in range(size_x):
        for j in range(size_y):
            for k in range(size_r):
                here = (i * size_y + j) * size_r + k
                there = ((i ^ flips[0]) * size_y + (j ^ flips[1])) * size_r + (k ^ flips[2])
                route.append((here, there))
    return lax.ppermute(array, ("gx", "gy", "row"), route)


def reduction_stages(mesh_sizes):
    size_x, size_y, _ = mesh_sizes
    stages = []
    bit = 1
    while bit < size_x:
        stages.append((bit, 0, 0))
        bit *= 2
    bit = 2
    while bit < size_y:
        stages.append((0, bit, 0))
        bit *= 2
    return stages


def chosen_rows(total, mesh_sizes):
    size_x, size_y, size_r = mesh_sizes
    stages = reduction_stages(mesh_sizes)
    unit = total // (size_x * size_y * size_r)
    blocks = 1 << len(stages)
    position = jnp.arange(blocks * unit, dtype=jnp.int32)
    place, inner = (position // unit, position % unit)
    x = jnp.zeros_like(position) + lax.axis_index("gx")
    y = jnp.zeros_like(position) + lax.axis_index("gy")
    for number, (bit_x, bit_y, _) in enumerate(stages):
        leaves = 1 - (place >> (len(stages) - 1 - number)) % 2
        x = x ^ (leaves * bit_x)
        y = y ^ (leaves * bit_y)
    block = (x * size_y + y) * size_r + lax.axis_index("row")
    return (block * unit + inner)[:, None]


def halved(leaving, staying, flips, mesh_sizes):
    arrived = exchange(leaving, mesh_sizes, flips)
    half = staying.shape[0] // 2
    return staying[:half] + arrived[:half], staying[half:] + arrived[half:]


def rest_halved(leaving, staying, stages, done, mesh_sizes):
    for number in range(done, len(stages) - 1):
        leaving, staying = halved(leaving, staying, stages[number], mesh_sizes)
    return staying + exchange(leaving, mesh_sizes, stages[-1])


def gelu_pair(values):
    root = math.sqrt(2.0 / math.pi)
    square = values * values
    bend = jnp.tanh(values * (root + (root * 0.044715) * square))
    cdf = 0.5 + 0.5 * bend
    slope = cdf + (0.5 * values) * (1.0 - bend * bend) * (root + (3.0 * root * 0.044715) * square)
    return values * cdf, slope


def gelu_value(values):
    root = math.sqrt(2.0 / math.pi)
    return values * (0.5 + 0.5 * jnp.tanh(values * (root + (root * 0.044715) * (values * values))))


def product(left, right):
    return jnp.dot(left, right, preferred_element_type=jnp.float32)


def product_transposed(left, right):
    return lax.dot_general(left, right, (((1,), (1,)), ((), ())), preferred_element_type=jnp.float32)


def transposed_choice(rows, source):
    columns = lax.broadcasted_iota(jnp.int32, (rows.shape[0], source.shape[1]), 1)
    choice = jnp.where(columns == rows, 1.0, 0.0).astype(jnp.bfloat16)
    return product_transposed(choice, source).astype(jnp.bfloat16)


def column_tiles(width):
    tile = 256 if width % 256 == 0 else width
    return [slice(start, start + tile) for start in range(0, width, tile)]


def store_halves(value, columns, leaving_ref, staying_ref):
    half = value.shape[0] // 2
    leaving_ref[:, columns] = value[:half]
    staying_ref[:, columns] = value[half:]


def forward_body(scale, own_ref, a_ref, b_ref, c_ref, first_ref, middle_ref, last_ref, rows_ref,
                 x_ref, h1_ref, s1_ref, h2_ref, s2_ref, error_ref, leaving_ref, staying_ref, first_near, last_near, semaphores):
    first_copy, last_copy = start_copies(((first_ref, first_near), (last_ref, last_near)), semaphores)
    count = own_ref.shape[0] // 2
    parts = (own_ref, a_ref, b_ref, c_ref)
    for number, part in enumerate(parts):
        x_ref[number * count:(number + 1) * count, :] = part[:count, :]
    x = x_ref[...]
    first_copy.wait()
    for columns in column_tiles(h1_ref.shape[1]):
        value, slope = gelu_pair(product(x, first_near[:, columns]))
        h1_ref[:, columns] = value.astype(jnp.bfloat16)
        s1_ref[:, columns] = slope
    h1 = h1_ref[...]
    for columns in column_tiles(h2_ref.shape[1]):
        value, slope = gelu_pair(product(h1, middle_ref[:, columns]))
        h2_ref[:, columns] = value.astype(jnp.bfloat16)
        s2_ref[:, columns] = slope
    h2 = h2_ref[...]
    last_copy.wait()
    for columns in column_tiles(error_ref.shape[1]):
        forcing = product(h2, last_near[:, columns])
        for number, part in enumerate(parts):
            block = slice(number * count, (number + 1) * count)
            target = part[count:, columns].astype(jnp.float32)
            error_ref[block, columns] = ((forcing[block] - target) * scale).astype(jnp.bfloat16)
    chosen = transposed_choice(rows_ref[...], h2)
    for columns in column_tiles(error_ref.shape[1]):
        store_halves(product(chosen, error_ref[:, columns]), columns, leaving_ref, staying_ref)


def backward_body(carried_ref, weight_ref, slope_ref, source_ref, rows_ref, back_ref, leaving_ref, staying_ref):
    carried = carried_ref[...]
    for columns in column_tiles(back_ref.shape[1]):
        value = product_transposed(carried, weight_ref[columns, :]) * slope_ref[:, columns]
        back_ref[:, columns] = value.astype(jnp.bfloat16)
    chosen = transposed_choice(rows_ref[...], source_ref[...])
    for columns in column_tiles(back_ref.shape[1]):
        store_halves(product(chosen, back_ref[:, columns]), columns, leaving_ref, staying_ref)


def tied(value, *others):
    return lax.optimization_barrier((value, *others))[0]


def kernel_call(body, outputs, scratch=(), flops=1 << 24, far=(), far_outputs=(), copies=0):
    def call(*inputs):
        near, away = (pl.BlockSpec(memory_space=pltpu.VMEM), pl.BlockSpec(memory_space=pltpu.HBM))
        result = pl.pallas_call(
            body,
            cost_estimate=pl.CostEstimate(flops=flops, transcendentals=0, bytes_accessed=0),
            in_specs=[away if number in far else near for number in range(len(inputs))],
            out_specs=[away if number in far_outputs else near for number in range(len(outputs))],
            out_shape=[(pltpu.HBM if number in far_outputs else jax.ShapeDtypeStruct)(shape, dtype)
                       for number, (shape, dtype) in enumerate(outputs)],
            scratch_shapes=[pltpu.VMEM(shape, dtype) for shape, dtype in scratch]
            + [pltpu.SemaphoreType.DMA((copies,))] * (copies > 0),
            compiler_params=pltpu.CompilerParams(vmem_limit_bytes=VMEM_LIMIT),
        )(*(pltpu.with_memory_space_constraint(array, pltpu.HBM) if number in far else array
            for number, array in enumerate(inputs)))
        return result

    return call


def all_steps(concentrations, diffusivity, weight_first, weight_middle, weight_last):
    mesh_sizes = tuple(lax.axis_size(axis) for axis in ("gx", "gy", "row"))
    length, height, width = diffusivity.shape
    f32, bf16 = (jnp.float32, jnp.bfloat16)
    planes, rows = (length + 2 * HALO, height + 2 * EDGE)
    wide = ((planes, 8 + rows + 8, 2 * width), f32)
    count = length * height * width // PATCH ** 3
    cells, hidden = weight_first.shape
    hidden_second = weight_middle.shape[1]
    total = 4 * count
    rows_first, rows_middle, rows_last = [chosen_rows(size, mesh_sizes) for size in (cells, hidden, hidden_second)]
    half_of = lambda chosen, width: ((chosen.shape[0] // 2, width), f32)
    stages = reduction_stages(mesh_sizes)
    big = 1 << 32

    layers = ((3 * HALO - 1, height, width), f32)
    weights = (weight_first, weight_middle, weight_last)
    leading, trailing, near_state, near_third = kernel_call(
        first_faces_body, [layers, layers, (concentrations.shape, f32), (diffusivity.shape, f32)],
        far=(0, 1), copies=2,
    )(concentrations, diffusivity)
    before, after = x_halos(leading, trailing)
    leading, trailing = edge_rows(near_state, near_third, before, after)
    below, above = y_halos(leading, trailing)
    whole, strips = assemble(near_state, near_third, before, after, below, above)
    state, own, wide_diffusivity = kernel_call(
        functools.partial(first_steps_body, PATCH),
        [(concentrations.shape, f32), ((2 * count, cells), bf16), wide],
        scratch=[wide] * 5 + [((length * height, width), f32)],
        far_outputs=(2,), copies=1,
    )(whole, *z_strips(strips))

    others = [exchange(own, mesh_sizes, flips) for flips in ((0, 0, 1), (0, 1, 0), (0, 1, 1))]
    (field,) = kernel_call(functools.partial(own_forward_body, PATCH), [(diffusivity.shape, f32)], flops=big // 4)(
        own, *weights
    )
    leading, trailing = kernel_call(store_faces, [layers, layers])(state, field)
    before, after = x_halos(leading, trailing)
    leading, trailing = edge_rows(state, field, before, after)
    below, above = y_halos(leading, trailing)
    x, h1, s1, h2, s2, error, *last = kernel_call(
        functools.partial(forward_body, 1.0 / count),
        [((total, cells), bf16), ((total, hidden), bf16), ((total, hidden), f32), ((total, hidden_second), bf16),
         ((total, hidden_second), f32), ((total, cells), bf16),
         half_of(rows_last, cells), half_of(rows_last, cells)],
        scratch=[(weight_first.shape, bf16), (weight_last.shape, bf16)],
        flops=big, far=(4, 6), copies=2,
    )(tied(own, leading, trailing), *others, *weights, rows_last)
    last = halved(*last, stages[0], mesh_sizes)
    whole, strips = assemble(state, field, before, after, tied(below, error), above)
    back_second, *middle = kernel_call(
        backward_body,
        [((total, hidden_second), bf16), half_of(rows_middle, hidden_second), half_of(rows_middle, hidden_second)],
        flops=big // 2,
    )(tied(error, strips, last[0]), weights[2], s2, h1, rows_middle)
    middle = halved(*middle, stages[0], mesh_sizes)
    last = halved(*last, stages[1], mesh_sizes)
    back_first, *first = kernel_call(
        backward_body,
        [((total, hidden), bf16), half_of(rows_first, hidden), half_of(rows_first, hidden)],
        flops=big // 2,
    )(tied(back_second, last[0], middle[0]), weights[1], s1, x, rows_first)
    first = halved(*first, stages[0], mesh_sizes)
    middle = halved(*middle, stages[1], mesh_sizes)
    (state,) = kernel_call(last_steps_body, [(state.shape, f32)], scratch=[wide] * 5, flops=big)(
        tied(whole, first[0], middle[0], last[0]), *z_strips(strips), wide_diffusivity
    )
    grads = [rest_halved(*part, stages, done, mesh_sizes) for part, done in ((first, 1), (middle, 2), (last, 2))]
    return (state, *grads)


def solution(mesh):
    in_specs = (P(None, "gx", "gy", "row"), P("gx", "gy", "row"), P(), P(), P())
    out_specs = (
        P(None, "gx", "gy", "row"),
        P(("gx", "gy", "row"), None),
        P(("gx", "gy", "row"), None),
        P(("gx", "gy", "row"), None),
    )
    return jax.shard_map(all_steps, mesh=mesh, in_specs=in_specs, out_specs=out_specs, check_vma=False)
```

```python
import functools
import math

import jax
import jax.numpy as jnp
from jax import lax
from jax.experimental import pallas as pl
from jax.experimental.pallas import tpu as pltpu
from jax.sharding import PartitionSpec as P

STEPS = 6
PATCH = 8
HALO = STEPS // 2
EDGE = 4
VMEM_LIMIT = 20 << 20


def ring(array, axis, distance):
    size = lax.axis_size(axis)
    return lax.ppermute(array, axis, [(i, (i + distance) % size) for i in range(size)])


def react(activator, inhibitor, diffusivity, lap_activator, lap_inhibitor, forcing):
    product = activator * inhibitor * inhibitor
    inner = diffusivity * lap_activator - product + 0.04 * (1.0 - activator)
    new_activator = activator + 0.1 * (inner if forcing is None else inner + forcing)
    new_inhibitor = inhibitor + 0.1 * (
        0.5 * diffusivity * lap_inhibitor + product - 0.1 * inhibitor
    )
    return (new_activator, new_inhibitor)


def fields(state, third):
    return ((lambda x, rows: state[0, x, rows, :], HALO), (lambda x, rows: state[1, x, rows, :], HALO),
            (lambda x, rows: third[x, rows, :], HALO - 1))


def plane_of(state, third, before, after, kind, plane, rows):
    read, depth = fields(state, third)[kind]
    length = state.shape[1]
    x = plane - HALO
    if x < -depth or x >= length + depth:
        return None
    if x < 0:
        return before[kind * HALO + depth + x, rows, :]
    if x >= length:
        return after[kind * HALO + x - length, rows, :]
    return read(x, rows)


def edge_rows_body(state, third, before, after, leading_ref, trailing_ref):
    length, height = state.shape[1:3]
    for plane in range(length + 2 * HALO):
        for kind, depth in enumerate((HALO, HALO, HALO - 1)):
            for out_ref, start in ((leading_ref, 0), (trailing_ref, height - depth)):
                value = plane_of(state, third, before, after, kind, plane, slice(start, start + depth))
                if value is None:
                    value = jnp.zeros((depth, state.shape[3]), jnp.float32)
                out_ref[plane, kind * HALO:kind * HALO + depth, :] = value


def strips_of(planes, width):
    each = width // (2 * HALO)
    places = {}
    for kind in range(3):
        for plane in range(kind // 2, planes - kind // 2):
            number = len(places)
            places[kind, plane] = (number // each, (number % each) * 2 * HALO)
    return places, -(-len(places) // each)


def assemble_body(state, third, before, after, below, above, whole_ref, strips_ref):
    length, height, width = state.shape[1:]
    planes = length + 2 * HALO
    places, _ = strips_of(planes, width)
    lanes = lax.broadcasted_iota(jnp.int32, whole_ref.shape[2:], 1)
    tiles = {}
    for kind, depth in enumerate((HALO, HALO, HALO - 1)):
        for plane in range(planes):
            value = plane_of(state, third, before, after, kind, plane, slice(0, height))
            if value is None:
                continue
            held = slice(kind * HALO, kind * HALO + depth)
            whole_ref[kind, plane, EDGE:EDGE + height, :] = value
            whole_ref[kind, plane, EDGE - depth:EDGE, :] = below[plane, held, :]
            whole_ref[kind, plane, EDGE + height:EDGE + height + depth, :] = above[plane, held, :]
            tile, shift = places[kind, plane]
            turned = pltpu.roll(whole_ref[kind, plane], (shift + HALO) % width, axis=1)
            here = (lanes >= shift) & (lanes < shift + 2 * HALO)
            tiles[tile] = jnp.where(here, turned, tiles[tile]) if tile in tiles else turned
    for tile, value in tiles.items():
        strips_ref[tile] = value


def load_sides(whole, earlier, later, kind, target, places, first):
    rows, width = whole.shape[2:]
    lanes = lax.broadcasted_iota(jnp.int32, (rows, width), 1)
    for plane in range(whole.shape[1]):
        if (kind, plane) not in places:
            continue
        tile, shift = places[kind, plane]
        back = (2 * width - shift - HALO) % width
        beside = later[tile] if later is earlier else jnp.where(
            (lanes >= shift + HALO) & (lanes < shift + 2 * HALO), later[tile], earlier[tile])
        target[plane, first:first + rows, :] = pltpu.roll(beside, back, axis=1)


def one_step(source, target, fixed, planes, rows, sides):
    def some_rows(plane, first):
        held, here = (slice(8 + first, 16 + first), slice(first, first + 8))
        around, centers = ([], [])
        for pair in source:
            summed, center = ([], [])
            for field in pair:
                middle = field[plane, held, :]
                total = -6.0 * middle + field[plane + 1, held, :] + field[plane - 1, held, :]
                summed.append(total + field[plane, 9 + first:17 + first, :] + field[plane, 7 + first:15 + first, :])
                center.append(middle)
            width = center[0].shape[1]
            lanes = lax.broadcasted_iota(jnp.int32, center[0].shape, 1)
            up = [pltpu.roll(value, 1, axis=1) for value in center]
            down = [pltpu.roll(value, width - 1, axis=1) for value in center]
            around.append([summed[n] + jnp.where(lanes == 0, up[1 - n], up[n])
                           + jnp.where(lanes == width - 1, down[1 - n], down[n]) for n in range(2)])
            centers.append(center)
        for n in range(2 if sides else 1):
            still = [pair[n][plane, here, :] for pair in fixed] + [None]
            new = react(centers[0][n], centers[1][n], still[0], around[0][n], around[1][n], still[1])
            for pair, value in zip(target, new):
                pair[n][plane, held, :] = value

    def one_plane(plane, carry):
        for first in range(0, rows, 8):
            some_rows(plane, first)
        return carry

    lax.fori_loop(planes[0], planes[1], one_plane, 0, unroll=True)


def run_steps(whole, earlier, later, fixed, now, then):
    places, _ = strips_of(whole.shape[1], whole.shape[3])
    planes, rows = whole.shape[1:3]
    for kind, pair in enumerate(now):
        load_sides(whole, earlier, later, kind, pair[1], places, 8)
        for plane in range(planes):
            pair[0][plane, 8:8 + rows, :] = whole[kind, plane]
    for step in range(HALO):
        one_step(now, then, fixed, (step + 1, planes - step - 1), rows, step < HALO - 1)
        now, then = then, now
    return now[0][0], now[1][0]


def move_order(patches_z, edge):
    lanes = patches_z * edge
    row = lax.broadcasted_iota(jnp.int32, (lanes, lanes), 0)
    column = lax.broadcasted_iota(jnp.int32, (lanes, lanes), 1)
    return jnp.where((row % patches_z) * edge + row // patches_z == column, 1.0, 0.0).astype(jnp.bfloat16)


def cell_order(edge):
    cells = edge ** 3
    row = lax.broadcasted_iota(jnp.int32, (cells, cells), 0)
    column = lax.broadcasted_iota(jnp.int32, (cells, cells), 1)
    return jnp.where((row % (edge * edge)) * edge + row // (edge * edge) == column, 1.0, 0.0).astype(jnp.bfloat16)


def half_tiles(source, count, rows, by_lane):
    half = by_lane // 2
    lanes = lax.broadcasted_iota(jnp.int32, (rows, by_lane), 1)
    out = []
    for b in range(count[1]):
        tiles = []
        for a in range(0, count[0], 2):
            low, high = [source[n * rows:(n + 1) * rows, (b // 2) * by_lane:(b // 2 + 1) * by_lane] for n in (a, a + 1)]
            if b % 2 == 0:
                high = pltpu.roll(high, half, axis=1)
            else:
                low = pltpu.roll(low, half, axis=1)
            tiles.append(jnp.where(lanes < half, low, high))
        out.append(jnp.concatenate(tiles, axis=1))
    return jnp.concatenate(out, axis=0)


def cube_starts(shape, edge):
    extent_x, extent_y = shape
    return [(px * edge + ix, py * edge) for px in range(extent_x // edge) for py in range(extent_y // edge)
            for ix in range(edge)]


def exact_product(left, right):
    high = left.astype(jnp.bfloat16)
    low = (left - high.astype(jnp.float32)).astype(jnp.bfloat16)
    return product(high, right) + product(low, right)


def paired(refs):
    pairs = list(zip(refs[::2], refs[1::2]))
    return pairs[:2], pairs[2:]


def first_steps_body(edge, whole, earlier, later, state_ref, own_ref, fixed_ref, *scratch):
    *fields_now, side, column_ref, semaphores = scratch
    length, height, width = state_ref.shape[1:]
    load_sides(whole, earlier, later, 2, side, strips_of(whole.shape[1], width)[0], 0)
    copies = start_copies([(whole.at[2], fixed_ref.at[0]), (side, fixed_ref.at[1])], semaphores)
    now = run_steps(whole, earlier, later, [(whole.at[2], side)], *paired(fields_now))
    move, order = (move_order(width // edge, edge), cell_order(edge))
    count = own_ref.shape[0] // 2
    for species, field in enumerate(now):
        for x in range(length):
            state_ref[species, x] = field[x + HALO, 8 + EDGE:8 + EDGE + height, :]
        for number, (x, y) in enumerate(cube_starts((length, height), edge)):
            column_ref[number * edge:(number + 1) * edge, :] = state_ref[species, x, y:y + edge, :]
        turned = product_transposed(move, column_ref[...].astype(jnp.bfloat16))
        columns = length * height // (edge * edge)
        cubes = half_tiles(turned, (edge, columns), width // edge, 2 * edge * edge)
        own_ref[species * count:(species + 1) * count, :] = product(cubes.astype(jnp.bfloat16), order).astype(jnp.bfloat16)
    for copy in copies:
        copy.wait()


def own_forward_body(edge, own_ref, first_ref, middle_ref, last_ref, field_ref):
    length, height, width = field_ref.shape
    count = own_ref.shape[0] // 2
    h1 = gelu_value(product(own_ref[:count, :], first_ref[...])).astype(jnp.bfloat16)
    h2 = gelu_value(product(h1, middle_ref[...])).astype(jnp.bfloat16)
    forcing = product(h2, last_ref[...])
    cells = lax.broadcasted_iota(jnp.int32, (edge ** 3, edge ** 3), 1)
    row = lax.broadcasted_iota(jnp.int32, (edge ** 3, edge ** 3), 0)
    square = edge * edge
    order = jnp.where((cells % square) * edge + cells // square == row, 1.0, 0.0).astype(jnp.bfloat16)
    columns = length * height // square
    turned = half_tiles(exact_product(forcing, order), (columns, edge), width // edge, 2 * square)
    moved = exact_product(turned.T, move_order(width // edge, edge))
    for number, (x, y) in enumerate(cube_starts((length, height), edge)):
        field_ref[x, y:y + edge, :] = moved[number * edge:(number + 1) * edge, :]


def last_steps_body(whole, earlier, later, fixed, state_ref, *scratch):
    *fields_now, side = scratch
    length, height, width = state_ref.shape[1:]
    load_sides(whole, earlier, later, 2, side, strips_of(whole.shape[1], width)[0], 0)
    both = [(fixed.at[0], fixed.at[1]), (whole.at[2], side)]
    now = run_steps(whole, earlier, later, both, *paired(fields_now))
    for species, field in enumerate(now):
        for x in range(length):
            state_ref[species, x] = field[x + HALO, 8 + EDGE:8 + EDGE + height, :]


def start_copies(pairs, semaphores):
    copies = [pltpu.make_async_copy(*pair, semaphores.at[number]) for number, pair in enumerate(pairs)]
    for copy in copies:
        copy.start()
    return copies


def store_faces(state, third, leading_ref, trailing_ref):
    length = third.shape[0]
    for kind, depth in enumerate((HALO, HALO, HALO - 1)):
        read = fields(state, third)[kind][0]
        for plane in range(depth):
            leading_ref[kind * HALO + plane] = read(plane, slice(None))
            trailing_ref[kind * HALO + plane] = read(length - depth + plane, slice(None))


def first_faces_body(state_ref, third_ref, leading_ref, trailing_ref, state_out, third_out, semaphores):
    for copy in start_copies(((state_ref, state_out), (third_ref, third_out)), semaphores):
        copy.wait()
    store_faces(state_out, third_out, leading_ref, trailing_ref)


def x_halos(leading, trailing):
    return ring(trailing, "gx", 1), ring(leading, "gx", -1)


def edge_rows(state, third, before, after):
    planes = state.shape[1] + 2 * HALO
    return kernel_call(edge_rows_body, [((planes, 3 * HALO - 1, state.shape[3]), jnp.float32)] * 2)(
        state, third, before, after
    )


def y_halos(leading, trailing):
    return ring(trailing, "gy", 1), ring(leading, "gy", -1)


def assemble(state, third, before, after, below, above):
    length, height, width = state.shape[1:]
    planes, rows = (length + 2 * HALO, height + 2 * EDGE)
    outputs = [(3, planes, rows, width), (strips_of(planes, width)[1], rows, width)]
    return kernel_call(assemble_body, [(shape, jnp.float32) for shape in outputs])(
        state, third, before, after, below, above
    )


def z_strips(strips):
    earlier = ring(strips, "row", 1)
    return earlier, (earlier if lax.axis_size("row") == 2 else ring(strips, "row", -1))


def exchange(array, mesh_sizes, flips):
    size_x, size_y, size_r = mesh_sizes
    route = []
    for i in range(size_x):
        for j in range(size_y):
            for k in range(size_r):
                here = (i * size_y + j) * size_r + k
                there = ((i ^ flips[0]) * size_y + (j ^ flips[1])) * size_r + (k ^ flips[2])
                route.append((here, there))
    return lax.ppermute(array, ("gx", "gy", "row"), route)


def reduction_stages(mesh_sizes):
    size_x, size_y, _ = mesh_sizes
    stages = []
    bit = 1
    while bit < size_x:
        stages.append((bit, 0, 0))
        bit *= 2
    bit = 2
    while bit < size_y:
        stages.append((0, bit, 0))
        bit *= 2
    return stages


def chosen_rows(total, mesh_sizes):
    size_x, size_y, size_r = mesh_sizes
    stages = reduction_stages(mesh_sizes)
    unit = total // (size_x * size_y * size_r)
    blocks = 1 << len(stages)
    position = jnp.arange(blocks * unit, dtype=jnp.int32)
    place, inner = (position // unit, position % unit)
    x = jnp.zeros_like(position) + lax.axis_index("gx")
    y = jnp.zeros_like(position) + lax.axis_index("gy")
    for number, (bit_x, bit_y, _) in enumerate(stages):
        leaves = 1 - (place >> (len(stages) - 1 - number)) % 2
        x = x ^ (leaves * bit_x)
        y = y ^ (leaves * bit_y)
    block = (x * size_y + y) * size_r + lax.axis_index("row")
    return (block * unit + inner)[:, None]


def halved(leaving, staying, flips, mesh_sizes):
    arrived = exchange(leaving, mesh_sizes, flips)
    half = staying.shape[0] // 2
    return staying[:half] + arrived[:half], staying[half:] + arrived[half:]


def rest_halved(leaving, staying, stages, done, mesh_sizes):
    for number in range(done, len(stages) - 1):
        leaving, staying = halved(leaving, staying, stages[number], mesh_sizes)
    return staying + exchange(leaving, mesh_sizes, stages[-1])


def gelu_pair(values):
    root = math.sqrt(2.0 / math.pi)
    square = values * values
    bend = jnp.tanh(values * (root + (root * 0.044715) * square))
    cdf = 0.5 + 0.5 * bend
    slope = cdf + (0.5 * values) * (1.0 - bend * bend) * (root + (3.0 * root * 0.044715) * square)
    return values * cdf, slope


def gelu_value(values):
    root = math.sqrt(2.0 / math.pi)
    return values * (0.5 + 0.5 * jnp.tanh(values * (root + (root * 0.044715) * (values * values))))


def product(left, right):
    return jnp.dot(left, right, preferred_element_type=jnp.float32)


def product_transposed(left, right):
    return lax.dot_general(left, right, (((1,), (1,)), ((), ())), preferred_element_type=jnp.float32)


def transposed_choice(rows, source):
    columns = lax.broadcasted_iota(jnp.int32, (rows.shape[0], source.shape[1]), 1)
    choice = jnp.where(columns == rows, 1.0, 0.0).astype(jnp.bfloat16)
    return product_transposed(choice, source).astype(jnp.bfloat16)


def column_tiles(width):
    tile = 256 if width % 256 == 0 else width
    return [slice(start, start + tile) for start in range(0, width, tile)]


def store_halves(value, columns, leaving_ref, staying_ref):
    half = value.shape[0] // 2
    leaving_ref[:, columns] = value[:half]
    staying_ref[:, columns] = value[half:]


def forward_body(scale, own_ref, a_ref, b_ref, c_ref, first_ref, middle_ref, last_ref, rows_ref,
                 x_ref, h1_ref, s1_ref, h2_ref, s2_ref, error_ref, leaving_ref, staying_ref, first_near, last_near, semaphores):
    first_copy, last_copy = start_copies(((first_ref, first_near), (last_ref, last_near)), semaphores)
    count = own_ref.shape[0] // 2
    parts = (own_ref, a_ref, b_ref, c_ref)
    for number, part in enumerate(parts):
        x_ref[number * count:(number + 1) * count, :] = part[:count, :]
    x = x_ref[...]
    first_copy.wait()
    for columns in column_tiles(h1_ref.shape[1]):
        value, slope = gelu_pair(product(x, first_near[:, columns]))
        h1_ref[:, columns] = value.astype(jnp.bfloat16)
        s1_ref[:, columns] = slope
    h1 = h1_ref[...]
    for columns in column_tiles(h2_ref.shape[1]):
        value, slope = gelu_pair(product(h1, middle_ref[:, columns]))
        h2_ref[:, columns] = value.astype(jnp.bfloat16)
        s2_ref[:, columns] = slope
    h2 = h2_ref[...]
    last_copy.wait()
    for columns in column_tiles(error_ref.shape[1]):
        forcing = product(h2, last_near[:, columns])
        for number, part in enumerate(parts):
            block = slice(number * count, (number + 1) * count)
            target = part[count:, columns].astype(jnp.float32)
            error_ref[block, columns] = ((forcing[block] - target) * scale).astype(jnp.bfloat16)
    chosen = transposed_choice(rows_ref[...], h2)
    for columns in column_tiles(error_ref.shape[1]):
        store_halves(product(chosen, error_ref[:, columns]), columns, leaving_ref, staying_ref)


def backward_body(carried_ref, weight_ref, slope_ref, source_ref, rows_ref, back_ref, leaving_ref, staying_ref):
    carried = carried_ref[...]
    for columns in column_tiles(back_ref.shape[1]):
        value = product_transposed(carried, weight_ref[columns, :]) * slope_ref[:, columns]
        back_ref[:, columns] = value.astype(jnp.bfloat16)
    chosen = transposed_choice(rows_ref[...], source_ref[...])
    for columns in column_tiles(back_ref.shape[1]):
        store_halves(product(chosen, back_ref[:, columns]), columns, leaving_ref, staying_ref)


def tied(value, *others):
    return lax.optimization_barrier((value, *others))[0]


def kernel_call(body, outputs, scratch=(), flops=1 << 24, far=(), far_outputs=(), copies=0):
    def call(*inputs):
        near, away = (pl.BlockSpec(memory_space=pltpu.VMEM), pl.BlockSpec(memory_space=pltpu.HBM))
        result = pl.pallas_call(
            body,
            cost_estimate=pl.CostEstimate(flops=flops, transcendentals=0, bytes_accessed=0),
            in_specs=[away if number in far else near for number in range(len(inputs))],
            out_specs=[away if number in far_outputs else near for number in range(len(outputs))],
            out_shape=[(pltpu.HBM if number in far_outputs else jax.ShapeDtypeStruct)(shape, dtype)
                       for number, (shape, dtype) in enumerate(outputs)],
            scratch_shapes=[pltpu.VMEM(shape, dtype) for shape, dtype in scratch]
            + [pltpu.SemaphoreType.DMA((copies,))] * (copies > 0),
            compiler_params=pltpu.CompilerParams(vmem_limit_bytes=VMEM_LIMIT),
        )(*(pltpu.with_memory_space_constraint(array, pltpu.HBM) if number in far else array
            for number, array in enumerate(inputs)))
        return result

    return call


def all_steps(concentrations, diffusivity, weight_first, weight_middle, weight_last):
    mesh_sizes = tuple(lax.axis_size(axis) for axis in ("gx", "gy", "row"))
    length, height, width = diffusivity.shape
    f32, bf16 = (jnp.float32, jnp.bfloat16)
    planes, rows = (length + 2 * HALO, height + 2 * EDGE)
    fixed = ((2, planes, rows, width), f32)
    buffers = [((planes, 8 + rows + 8, width), f32)] * 8 + [((planes, rows, width), f32)]
    count = length * height * width // PATCH ** 3
    cells, hidden = weight_first.shape
    hidden_second = weight_middle.shape[1]
    total = 4 * count
    rows_first, rows_middle, rows_last = [chosen_rows(size, mesh_sizes) for size in (cells, hidden, hidden_second)]
    half_of = lambda chosen, width: ((chosen.shape[0] // 2, width), f32)
    stages = reduction_stages(mesh_sizes)
    big = 1 << 32

    layers = ((3 * HALO - 1, height, width), f32)
    weights = (weight_first, weight_middle, weight_last)
    leading, trailing, near_state, near_third = kernel_call(
        first_faces_body, [layers, layers, (concentrations.shape, f32), (diffusivity.shape, f32)],
        far=(0, 1), copies=2,
    )(concentrations, diffusivity)
    before, after = x_halos(leading, trailing)
    leading, trailing = edge_rows(near_state, near_third, before, after)
    below, above = y_halos(leading, trailing)
    whole, strips = assemble(near_state, near_third, before, after, below, above)
    state, own, diffusivity_fixed = kernel_call(
        functools.partial(first_steps_body, PATCH),
        [(concentrations.shape, f32), ((2 * count, cells), bf16), fixed],
        scratch=buffers + [((length * height, width), f32)],
        far_outputs=(2,), copies=2,
    )(whole, *z_strips(strips))

    others = [exchange(own, mesh_sizes, flips) for flips in ((0, 0, 1), (0, 1, 0), (0, 1, 1))]
    (field,) = kernel_call(functools.partial(own_forward_body, PATCH), [(diffusivity.shape, f32)], flops=big // 4)(
        own, *weights
    )
    leading, trailing = kernel_call(store_faces, [layers, layers])(state, field)
    before, after = x_halos(leading, trailing)
    leading, trailing = edge_rows(state, field, before, after)
    below, above = y_halos(leading, trailing)
    x, h1, s1, h2, s2, error, *last = kernel_call(
        functools.partial(forward_body, 1.0 / count),
        [((total, cells), bf16), ((total, hidden), bf16), ((total, hidden), f32), ((total, hidden_second), bf16),
         ((total, hidden_second), f32), ((total, cells), bf16),
         half_of(rows_last, cells), half_of(rows_last, cells)],
        scratch=[(weight_first.shape, bf16), (weight_last.shape, bf16)],
        flops=big, far=(4, 6), copies=2,
    )(tied(own, leading, trailing), *others, *weights, rows_last)
    last = halved(*last, stages[0], mesh_sizes)
    whole, strips = assemble(state, field, before, after, tied(below, error), above)
    back_second, *middle = kernel_call(
        backward_body,
        [((total, hidden_second), bf16), half_of(rows_middle, hidden_second), half_of(rows_middle, hidden_second)],
        flops=big // 2,
    )(tied(error, strips, last[0]), weights[2], s2, h1, rows_middle)
    middle = halved(*middle, stages[0], mesh_sizes)
    last = halved(*last, stages[1], mesh_sizes)
    back_first, *first = kernel_call(
        backward_body,
        [((total, hidden), bf16), half_of(rows_first, hidden), half_of(rows_first, hidden)],
        flops=big // 2,
    )(tied(back_second, last[0], middle[0]), weights[1], s1, x, rows_first)
    first = halved(*first, stages[0], mesh_sizes)
    middle = halved(*middle, stages[1], mesh_sizes)
    (state,) = kernel_call(last_steps_body, [(state.shape, f32)], scratch=buffers, flops=big)(
        tied(whole, first[0], middle[0], last[0]), *z_strips(strips), diffusivity_fixed
    )
    grads = [rest_halved(*part, stages, done, mesh_sizes) for part, done in ((first, 1), (middle, 2), (last, 2))]
    return (state, *grads)


def solution(mesh):
    in_specs = (P(None, "gx", "gy", "row"), P("gx", "gy", "row"), P(), P(), P())
    out_specs = (
        P(None, "gx", "gy", "row"),
        P(("gx", "gy", "row"), None),
        P(("gx", "gy", "row"), None),
        P(("gx", "gy", "row"), None),
    )
    return jax.shard_map(all_steps, mesh=mesh, in_specs=in_specs, out_specs=out_specs, check_vma=False)
```

```python
import functools
import math

import jax
import jax.numpy as jnp
from jax import lax
from jax.experimental import pallas as pl
from jax.experimental.pallas import tpu as pltpu
from jax.sharding import PartitionSpec as P

STEPS = 6
PATCH = 8
HALO = STEPS // 2
EDGE = 4
VMEM_LIMIT = 20 << 20


def ring(array, axis, distance):
    size = lax.axis_size(axis)
    return lax.ppermute(array, axis, [(i, (i + distance) % size) for i in range(size)])


def react(activator, inhibitor, diffusivity, lap_activator, lap_inhibitor, forcing):
    product = activator * inhibitor * inhibitor
    inner = diffusivity * lap_activator - product + 0.04 * (1.0 - activator)
    new_activator = activator + 0.1 * (inner if forcing is None else inner + forcing)
    new_inhibitor = inhibitor + 0.1 * (
        0.5 * diffusivity * lap_inhibitor + product - 0.1 * inhibitor
    )
    return (new_activator, new_inhibitor)


def fields(state, third):
    return ((lambda x, rows: state[0, x, rows, :], HALO), (lambda x, rows: state[1, x, rows, :], HALO),
            (lambda x, rows: third[x, rows, :], HALO - 1))


def plane_of(state, third, before, after, kind, plane, rows):
    read, depth = fields(state, third)[kind]
    length = state.shape[1]
    x = plane - HALO
    if x < -depth or x >= length + depth:
        return None
    if x < 0:
        return before[kind * HALO + depth + x, rows, :]
    if x >= length:
        return after[kind * HALO + x - length, rows, :]
    return read(x, rows)


def edge_rows_body(state, third, before, after, leading_ref, trailing_ref):
    length, height = state.shape[1:3]
    for plane in range(length + 2 * HALO):
        for kind, depth in enumerate((HALO, HALO, HALO - 1)):
            for out_ref, start in ((leading_ref, 0), (trailing_ref, height - depth)):
                value = plane_of(state, third, before, after, kind, plane, slice(start, start + depth))
                if value is None:
                    value = jnp.zeros((depth, state.shape[3]), jnp.float32)
                out_ref[plane, kind * HALO:kind * HALO + depth, :] = value


def strips_of(planes, width):
    each = width // (2 * HALO)
    places = {}
    for kind in range(3):
        for plane in range(kind // 2, planes - kind // 2):
            number = len(places)
            places[kind, plane] = (number // each, (number % each) * 2 * HALO)
    return places, -(-len(places) // each)


def assemble_body(state, third, before, after, below, above, whole_ref, strips_ref):
    length, height, width = state.shape[1:]
    planes = length + 2 * HALO
    places, _ = strips_of(planes, width)
    lanes = lax.broadcasted_iota(jnp.int32, whole_ref.shape[2:], 1)
    tiles = {}
    for kind, depth in enumerate((HALO, HALO, HALO - 1)):
        for plane in range(planes):
            value = plane_of(state, third, before, after, kind, plane, slice(0, height))
            if value is None:
                continue
            held = slice(kind * HALO, kind * HALO + depth)
            whole_ref[kind, plane, EDGE:EDGE + height, :] = value
            whole_ref[kind, plane, EDGE - depth:EDGE, :] = below[plane, held, :]
            whole_ref[kind, plane, EDGE + height:EDGE + height + depth, :] = above[plane, held, :]
            tile, shift = places[kind, plane]
            turned = pltpu.roll(whole_ref[kind, plane], (shift + HALO) % width, axis=1)
            here = (lanes >= shift) & (lanes < shift + 2 * HALO)
            tiles[tile] = jnp.where(here, turned, tiles[tile]) if tile in tiles else turned
    for tile, value in tiles.items():
        strips_ref[tile] = value


def load_sides(whole, earlier, later, kind, target, places, first):
    rows, width = whole.shape[2:]
    lanes = lax.broadcasted_iota(jnp.int32, (rows, width), 1)
    for plane in range(whole.shape[1]):
        if (kind, plane) not in places:
            continue
        tile, shift = places[kind, plane]
        back = (2 * width - shift - HALO) % width
        beside = later[tile] if later is earlier else jnp.where(
            (lanes >= shift + HALO) & (lanes < shift + 2 * HALO), later[tile], earlier[tile])
        target[plane, first:first + rows, :] = pltpu.roll(beside, back, axis=1)


def one_step(source, target, fixed, planes, rows, sides):
    def some_rows(plane, first):
        held, here = (slice(8 + first, 16 + first), slice(first, first + 8))
        around, centers = ([], [])
        for pair in source:
            summed, center = ([], [])
            for field in pair:
                middle = field[plane, held, :]
                total = -6.0 * middle + field[plane + 1, held, :] + field[plane - 1, held, :]
                summed.append(total + field[plane, 9 + first:17 + first, :] + field[plane, 7 + first:15 + first, :])
                center.append(middle)
            width = center[0].shape[1]
            lanes = lax.broadcasted_iota(jnp.int32, center[0].shape, 1)
            up = [pltpu.roll(value, 1, axis=1) for value in center]
            down = [pltpu.roll(value, width - 1, axis=1) for value in center]
            around.append([summed[n] + jnp.where(lanes == 0, up[1 - n], up[n])
                           + jnp.where(lanes == width - 1, down[1 - n], down[n]) for n in range(2)])
            centers.append(center)
        for n in range(2 if sides else 1):
            still = [pair[n][plane, here, :] for pair in fixed] + [None]
            new = react(centers[0][n], centers[1][n], still[0], around[0][n], around[1][n], still[1])
            for pair, value in zip(target, new):
                pair[n][plane, held, :] = value

    def one_plane(plane, carry):
        for first in range(0, rows, 8):
            some_rows(plane, first)
        return carry

    lax.fori_loop(planes[0], planes[1], one_plane, 0, unroll=True)


def run_steps(whole, earlier, later, fixed, now, then):
    places, _ = strips_of(whole.shape[1], whole.shape[3])
    planes, rows = whole.shape[1:3]
    for kind, pair in enumerate(now):
        load_sides(whole, earlier, later, kind, pair[1], places, 8)
        for plane in range(planes):
            pair[0][plane, 8:8 + rows, :] = whole[kind, plane]
    for step in range(HALO):
        one_step(now, then, fixed, (step + 1, planes - step - 1), rows, step < HALO - 1)
        now, then = then, now
    return now[0][0], now[1][0]


def move_order(patches_z, edge):
    lanes = patches_z * edge
    row = lax.broadcasted_iota(jnp.int32, (lanes, lanes), 0)
    column = lax.broadcasted_iota(jnp.int32, (lanes, lanes), 1)
    return jnp.where((row % patches_z) * edge + row // patches_z == column, 1.0, 0.0).astype(jnp.bfloat16)


def cell_order(edge):
    cells = edge ** 3
    row = lax.broadcasted_iota(jnp.int32, (cells, cells), 0)
    column = lax.broadcasted_iota(jnp.int32, (cells, cells), 1)
    return jnp.where((row % (edge * edge)) * edge + row // (edge * edge) == column, 1.0, 0.0).astype(jnp.bfloat16)


def half_tiles(source, count, rows, by_lane):
    half = by_lane // 2
    lanes = lax.broadcasted_iota(jnp.int32, (rows, by_lane), 1)
    out = []
    for b in range(count[1]):
        tiles = []
        for a in range(0, count[0], 2):
            low, high = [source[n * rows:(n + 1) * rows, (b // 2) * by_lane:(b // 2 + 1) * by_lane] for n in (a, a + 1)]
            if b % 2 == 0:
                high = pltpu.roll(high, half, axis=1)
            else:
                low = pltpu.roll(low, half, axis=1)
            tiles.append(jnp.where(lanes < half, low, high))
        out.append(jnp.concatenate(tiles, axis=1))
    return jnp.concatenate(out, axis=0)


def cube_starts(shape, edge):
    extent_x, extent_y = shape
    return [(px * edge + ix, py * edge) for px in range(extent_x // edge) for py in range(extent_y // edge)
            for ix in range(edge)]


def exact_product(left, right):
    high = left.astype(jnp.bfloat16)
    low = (left - high.astype(jnp.float32)).astype(jnp.bfloat16)
    return product(high, right) + product(low, right)


def paired(refs):
    pairs = list(zip(refs[::2], refs[1::2]))
    return pairs[:2], pairs[2:]


def first_steps_body(edge, whole, earlier, later, state_ref, inputs_ref, targets_ref, fixed_ref, *scratch):
    *fields_now, side, column_ref, semaphores = scratch
    length, height, width = state_ref.shape[1:]
    load_sides(whole, earlier, later, 2, side, strips_of(whole.shape[1], width)[0], 0)
    copies = start_copies([(whole.at[2], fixed_ref.at[0]), (side, fixed_ref.at[1])], semaphores)
    now = run_steps(whole, earlier, later, [(whole.at[2], side)], *paired(fields_now))
    move, order = (move_order(width // edge, edge), cell_order(edge))
    for species, (field, out_ref) in enumerate(zip(now, (inputs_ref, targets_ref))):
        for x in range(length):
            state_ref[species, x] = field[x + HALO, 8 + EDGE:8 + EDGE + height, :]
        for number, (x, y) in enumerate(cube_starts((length, height), edge)):
            column_ref[number * edge:(number + 1) * edge, :] = state_ref[species, x, y:y + edge, :]
        turned = product_transposed(move, column_ref[...].astype(jnp.bfloat16))
        columns = length * height // (edge * edge)
        cubes = half_tiles(turned, (edge, columns), width // edge, 2 * edge * edge)
        out_ref[...] = product(cubes.astype(jnp.bfloat16), order).astype(jnp.bfloat16)
    for copy in copies:
        copy.wait()


def own_forward_body(edge, inputs_ref, first_ref, middle_ref, last_ref, field_ref):
    length, height, width = field_ref.shape
    h1 = gelu_value(product(inputs_ref[...], first_ref[...])).astype(jnp.bfloat16)
    h2 = gelu_value(product(h1, middle_ref[...])).astype(jnp.bfloat16)
    forcing = product(h2, last_ref[...])
    cells = lax.broadcasted_iota(jnp.int32, (edge ** 3, edge ** 3), 1)
    row = lax.broadcasted_iota(jnp.int32, (edge ** 3, edge ** 3), 0)
    square = edge * edge
    order = jnp.where((cells % square) * edge + cells // square == row, 1.0, 0.0).astype(jnp.bfloat16)
    columns = length * height // square
    turned = half_tiles(exact_product(forcing, order), (columns, edge), width // edge, 2 * square)
    moved = exact_product(turned.T, move_order(width // edge, edge))
    for number, (x, y) in enumerate(cube_starts((length, height), edge)):
        field_ref[x, y:y + edge, :] = moved[number * edge:(number + 1) * edge, :]


def last_steps_body(whole, earlier, later, fixed, state_ref, *scratch):
    *fields_now, side = scratch
    length, height, width = state_ref.shape[1:]
    load_sides(whole, earlier, later, 2, side, strips_of(whole.shape[1], width)[0], 0)
    both = [(fixed.at[0], fixed.at[1]), (whole.at[2], side)]
    now = run_steps(whole, earlier, later, both, *paired(fields_now))
    for species, field in enumerate(now):
        for x in range(length):
            state_ref[species, x] = field[x + HALO, 8 + EDGE:8 + EDGE + height, :]


def start_copies(pairs, semaphores):
    copies = [pltpu.make_async_copy(*pair, semaphores.at[number]) for number, pair in enumerate(pairs)]
    for copy in copies:
        copy.start()
    return copies


def bring_body(far_ref, near_ref, semaphores):
    start_copies([(far_ref, near_ref)], semaphores)[0].wait()


def store_faces(state, third, leading_ref, trailing_ref):
    length = third.shape[0]
    for kind, depth in enumerate((HALO, HALO, HALO - 1)):
        read = fields(state, third)[kind][0]
        for plane in range(depth):
            leading_ref[kind * HALO + plane] = read(plane, slice(None))
            trailing_ref[kind * HALO + plane] = read(length - depth + plane, slice(None))


def first_faces_body(state_ref, third_ref, leading_ref, trailing_ref, state_out, third_out, semaphores):
    for copy in start_copies(((state_ref, state_out), (third_ref, third_out)), semaphores):
        copy.wait()
    store_faces(state_out, third_out, leading_ref, trailing_ref)


def x_halos(leading, trailing):
    return ring(trailing, "gx", 1), ring(leading, "gx", -1)


def edge_rows(state, third, before, after):
    planes = state.shape[1] + 2 * HALO
    return kernel_call(edge_rows_body, [((planes, 3 * HALO - 1, state.shape[3]), jnp.float32)] * 2)(
        state, third, before, after
    )


def y_halos(leading, trailing):
    return ring(trailing, "gy", 1), ring(leading, "gy", -1)


def assemble(state, third, before, after, below, above):
    length, height, width = state.shape[1:]
    planes, rows = (length + 2 * HALO, height + 2 * EDGE)
    outputs = [(3, planes, rows, width), (strips_of(planes, width)[1], rows, width)]
    return kernel_call(assemble_body, [(shape, jnp.float32) for shape in outputs])(
        state, third, before, after, below, above
    )


def z_strips(strips):
    earlier = ring(strips, "row", 1)
    return earlier, (earlier if lax.axis_size("row") == 2 else ring(strips, "row", -1))


def exchange(array, mesh_sizes, flips):
    size_x, size_y, size_r = mesh_sizes
    route = []
    for i in range(size_x):
        for j in range(size_y):
            for k in range(size_r):
                here = (i * size_y + j) * size_r + k
                there = ((i ^ flips[0]) * size_y + (j ^ flips[1])) * size_r + (k ^ flips[2])
                route.append((here, there))
    return lax.ppermute(array, ("gx", "gy", "row"), route)


def reduction_stages(mesh_sizes):
    size_x, size_y, _ = mesh_sizes
    stages = []
    bit = 1
    while bit < size_x:
        stages.append((bit, 0, 0))
        bit *= 2
    bit = 2
    while bit < size_y:
        stages.append((0, bit, 0))
        bit *= 2
    return stages


def chosen_rows(total, mesh_sizes):
    size_x, size_y, size_r = mesh_sizes
    stages = reduction_stages(mesh_sizes)
    unit = total // (size_x * size_y * size_r)
    blocks = 1 << len(stages)
    position = jnp.arange(blocks * unit, dtype=jnp.int32)
    place, inner = (position // unit, position % unit)
    x = jnp.zeros_like(position) + lax.axis_index("gx")
    y = jnp.zeros_like(position) + lax.axis_index("gy")
    for number, (bit_x, bit_y, _) in enumerate(stages):
        leaves = 1 - (place >> (len(stages) - 1 - number)) % 2
        x = x ^ (leaves * bit_x)
        y = y ^ (leaves * bit_y)
    block = (x * size_y + y) * size_r + lax.axis_index("row")
    return (block * unit + inner)[:, None]


def halved(leaving, staying, flips, mesh_sizes):
    arrived = exchange(leaving, mesh_sizes, flips)
    half = staying.shape[0] // 2
    return staying[:half] + arrived[:half], staying[half:] + arrived[half:]


def rest_halved(leaving, staying, stages, done, mesh_sizes):
    for number in range(done, len(stages) - 1):
        leaving, staying = halved(leaving, staying, stages[number], mesh_sizes)
    arrived = exchange(leaving, mesh_sizes, stages[-1])
    return staying + arrived


def gelu_pair(values):
    root = math.sqrt(2.0 / math.pi)
    square = values * values
    bend = jnp.tanh(values * (root + (root * 0.044715) * square))
    cdf = 0.5 + 0.5 * bend
    slope = cdf + (0.5 * values) * (1.0 - bend * bend) * (root + (3.0 * root * 0.044715) * square)
    return values * cdf, slope


def gelu_value(values):
    root = math.sqrt(2.0 / math.pi)
    return values * (0.5 + 0.5 * jnp.tanh(values * (root + (root * 0.044715) * (values * values))))


def product(left, right):
    return jnp.dot(left, right, preferred_element_type=jnp.float32)


def product_transposed(left, right):
    return lax.dot_general(left, right, (((1,), (1,)), ((), ())), preferred_element_type=jnp.float32)


def transposed_choice(rows, source):
    columns = lax.broadcasted_iota(jnp.int32, (rows.shape[0], source.shape[1]), 1)
    choice = jnp.where(columns == rows, 1.0, 0.0).astype(jnp.bfloat16)
    return product_transposed(choice, source).astype(jnp.bfloat16)


def column_tiles(width):
    tile = 256 if width % 256 == 0 else width
    return [slice(start, start + tile) for start in range(0, width, tile)]


def store_halves(value, columns, leaving_ref, staying_ref):
    half = value.shape[0] // 2
    leaving_ref[:, columns] = value[:half]
    staying_ref[:, columns] = value[half:]


def activated(left, weight, value_ref, slope_ref):
    tiles = column_tiles(value_ref.shape[1])
    ahead = product(left, weight[:, tiles[0]])
    for number, columns in enumerate(tiles):
        now = ahead
        if number + 1 < len(tiles):
            ahead = product(left, weight[:, tiles[number + 1]])
        value, slope = gelu_pair(now)
        value_ref[:, columns] = value.astype(jnp.bfloat16)
        slope_ref[:, columns] = slope


def forward_one_body(own_ref, a_ref, b_ref, c_ref, first_ref, middle_ref,
                     x_ref, h1_ref, s1_ref, h2_ref, s2_ref):
    count = own_ref.shape[0]
    for number, part in enumerate((own_ref, a_ref, b_ref, c_ref)):
        x_ref[number * count:(number + 1) * count, :] = part[...]
    activated(x_ref[...], first_ref, h1_ref, s1_ref)
    activated(h1_ref[...], middle_ref, h2_ref, s2_ref)


def forward_two_body(scale, h2_ref, own_ref, a_ref, b_ref, c_ref, last_ref, rows_ref, error_ref, leaving_ref, staying_ref):
    count = own_ref.shape[0]
    h2 = h2_ref[...]
    for columns in column_tiles(error_ref.shape[1]):
        forcing = product(h2, last_ref[:, columns])
        for number, part in enumerate((own_ref, a_ref, b_ref, c_ref)):
            block = slice(number * count, (number + 1) * count)
            target = part[:, columns].astype(jnp.float32)
            error_ref[block, columns] = ((forcing[block] - target) * scale).astype(jnp.bfloat16)
    chosen = transposed_choice(rows_ref[...], h2)
    for columns in column_tiles(error_ref.shape[1]):
        store_halves(product(chosen, error_ref[:, columns]), columns, leaving_ref, staying_ref)


def backward_body(carried_ref, weight_ref, slope_ref, source_ref, rows_ref, back_ref, leaving_ref, staying_ref):
    carried = carried_ref[...]
    for columns in column_tiles(back_ref.shape[1]):
        value = product_transposed(carried, weight_ref[columns, :]) * slope_ref[:, columns]
        back_ref[:, columns] = value.astype(jnp.bfloat16)
    chosen = transposed_choice(rows_ref[...], source_ref[...])
    for columns in column_tiles(back_ref.shape[1]):
        store_halves(product(chosen, back_ref[:, columns]), columns, leaving_ref, staying_ref)


def tied(value, *others):
    return lax.optimization_barrier((value, *others))[0]


def kernel_call(body, outputs, scratch=(), flops=1 << 31, far=(), far_outputs=(), copies=0):
    def call(*inputs):
        near, away = (pl.BlockSpec(memory_space=pltpu.VMEM), pl.BlockSpec(memory_space=pltpu.HBM))
        result = pl.pallas_call(
            body,
            cost_estimate=pl.CostEstimate(flops=flops, transcendentals=0, bytes_accessed=0),
            in_specs=[away if number in far else near for number in range(len(inputs))],
            out_specs=[away if number in far_outputs else near for number in range(len(outputs))],
            out_shape=[(pltpu.HBM if number in far_outputs else jax.ShapeDtypeStruct)(shape, dtype)
                       for number, (shape, dtype) in enumerate(outputs)],
            scratch_shapes=[pltpu.VMEM(shape, dtype) for shape, dtype in scratch]
            + [pltpu.SemaphoreType.DMA((copies,))] * (copies > 0),
            compiler_params=pltpu.CompilerParams(vmem_limit_bytes=VMEM_LIMIT),
        )(*(pltpu.with_memory_space_constraint(array, pltpu.HBM) if number in far else array
            for number, array in enumerate(inputs)))
        return result

    return call


def all_steps(concentrations, diffusivity, weight_first, weight_middle, weight_last):
    mesh_sizes = tuple(lax.axis_size(axis) for axis in ("gx", "gy", "row"))
    length, height, width = diffusivity.shape
    f32, bf16 = (jnp.float32, jnp.bfloat16)
    planes, rows = (length + 2 * HALO, height + 2 * EDGE)
    fixed = ((2, planes, rows, width), f32)
    buffers = [((planes, 8 + rows + 8, width), f32)] * 8 + [((planes, rows, width), f32)]
    count = length * height * width // PATCH ** 3
    cells, hidden = weight_first.shape
    hidden_second = weight_middle.shape[1]
    total = 4 * count
    rows_first, rows_middle, rows_last = [chosen_rows(size, mesh_sizes) for size in (cells, hidden, hidden_second)]
    half_of = lambda chosen, width: ((chosen.shape[0] // 2, width), f32)
    stages = reduction_stages(mesh_sizes)
    big = 1 << 32

    layers = ((3 * HALO - 1, height, width), f32)
    leading, trailing, near_state, near_third = kernel_call(
        first_faces_body, [layers, layers, (concentrations.shape, f32), (diffusivity.shape, f32)],
        far=(0, 1), copies=2,
    )(concentrations, diffusivity)
    before, after = x_halos(leading, trailing)
    (near_last,) = kernel_call(bring_body, [(weight_last.shape, bf16)], far=(0,), copies=1)(weight_last)
    leading, trailing = edge_rows(near_state, near_third, before, after)
    below, above = y_halos(leading, trailing)
    whole, strips = assemble(near_state, near_third, before, after, below, above)
    state, inputs, targets, diffusivity_fixed = kernel_call(
        functools.partial(first_steps_body, PATCH),
        [(concentrations.shape, f32), ((count, cells), bf16), ((count, cells), bf16), fixed],
        scratch=buffers + [((length * height, width), f32)],
        far_outputs=(3,), copies=2,
    )(whole, *z_strips(strips))

    gather = lambda array: [exchange(array, mesh_sizes, flips) for flips in ((0, 0, 1), (0, 1, 0), (0, 1, 1))]
    all_inputs = gather(inputs)
    (field,) = kernel_call(functools.partial(own_forward_body, PATCH), [(diffusivity.shape, f32)],
        flops=big // 4,
    )(
        inputs, weight_first, weight_middle, near_last
    )
    all_targets = gather(tied(targets, field))
    leading, trailing = kernel_call(store_faces, [layers, layers])(state, field)
    before, after = x_halos(leading, trailing)
    x, h1, s1, h2, s2 = kernel_call(
        forward_one_body,
        [((total, cells), bf16), ((total, hidden), bf16), ((total, hidden), f32), ((total, hidden_second), bf16),
         ((total, hidden_second), f32)],
        flops=big,
    )(tied(inputs, leading, trailing), *all_inputs, weight_first, weight_middle)
    leading, trailing = edge_rows(state, field, tied(before, h2), after)
    below, above = y_halos(leading, trailing)
    error, *last = kernel_call(
        functools.partial(forward_two_body, 1.0 / count),
        [((total, cells), bf16), half_of(rows_last, cells), half_of(rows_last, cells)],
        flops=big,
    )(tied(h2, leading, trailing), targets, *all_targets, weight_last, rows_last)
    last = halved(*last, stages[0], mesh_sizes)
    back_second, *middle = kernel_call(
        backward_body,
        [((total, hidden_second), bf16), half_of(rows_middle, hidden_second), half_of(rows_middle, hidden_second)],
        flops=big // 2,
    )(error, weight_last, s2, h1, rows_middle)
    middle = halved(*middle, stages[0], mesh_sizes)
    last_leaving = last[0]
    whole, strips = assemble(state, field, before, after, tied(below, back_second, last_leaving, middle[0]), above)
    last = halved(*last, stages[1], mesh_sizes)
    back_first, *first = kernel_call(
        backward_body,
        [((total, hidden), bf16), half_of(rows_first, hidden), half_of(rows_first, hidden)],
        flops=big // 2,
    )(tied(back_second, strips), weight_middle, s1, x, rows_first)
    first = halved(*first, stages[0], mesh_sizes)
    middle = halved(*middle, stages[1], mesh_sizes)
    (state,) = kernel_call(last_steps_body, [(state.shape, f32)], scratch=buffers, flops=big)(
        tied(whole, first[0], middle[0], last[0]), *z_strips(strips), diffusivity_fixed
    )
    grads = [rest_halved(*part, stages, done, mesh_sizes) for part, done in ((first, 1), (middle, 2), (last, 2))]
    return (state, *grads)


def solution(mesh):
    in_specs = (P(None, "gx", "gy", "row"), P("gx", "gy", "row"), P(), P(), P())
    out_specs = (
        P(None, "gx", "gy", "row"),
        P(("gx", "gy", "row"), None),
        P(("gx", "gy", "row"), None),
        P(("gx", "gy", "row"), None),
    )
    return jax.shard_map(all_steps, mesh=mesh, in_specs=in_specs, out_specs=out_specs, check_vma=False)
```

```python
import functools
import math

import jax
import jax.numpy as jnp
from jax import lax
from jax.experimental import pallas as pl
from jax.experimental.pallas import tpu as pltpu
from jax.sharding import PartitionSpec as P

STEPS = 6
PATCH = 8
HALO = STEPS // 2
EDGE = 4
VMEM_LIMIT = 20 << 20


def ring(array, axis, distance):
    size = lax.axis_size(axis)
    return lax.ppermute(array, axis, [(i, (i + distance) % size) for i in range(size)])


def react(activator, inhibitor, diffusivity, lap_activator, lap_inhibitor, forcing):
    product = activator * inhibitor * inhibitor
    inner = diffusivity * lap_activator - product + 0.04 * (1.0 - activator)
    new_activator = activator + 0.1 * (inner if forcing is None else inner + forcing)
    new_inhibitor = inhibitor + 0.1 * (
        0.5 * diffusivity * lap_inhibitor + product - 0.1 * inhibitor
    )
    return (new_activator, new_inhibitor)


def fields(state, third):
    return ((lambda x, rows: state[0, x, rows, :], HALO), (lambda x, rows: state[1, x, rows, :], HALO),
            (lambda x, rows: third[x, rows, :], HALO - 1))


LAYERS = 3 * HALO - 1
PACKED = LAYERS + 2


def rounded(value):
    return value.astype(jnp.bfloat16).astype(jnp.float32)


def whole_tiles(rows):
    return -(-rows // 16) * 16


def plane_of(state, third, before, after, kind, plane, rows):
    read, depth = fields(state, third)[kind]
    length = state.shape[1]
    x = plane - HALO
    if x < -depth or x >= length + depth:
        return None
    if 0 <= x < length:
        return read(x, rows)
    halo, layer = (before, kind * HALO + depth + x) if x < 0 else (after, kind * HALO + x - length)
    value = halo[layer].astype(jnp.float32)
    if kind < 2 and x in (-1, length):
        value = value + halo[LAYERS + kind].astype(jnp.float32)
    return value[rows]


def edge_rows_body(state, third, before, after, leading_ref, trailing_ref, leading, trailing):
    length, height, width = state.shape[1:]
    planes = length + 2 * HALO
    for side, start_of, nearest in ((leading, lambda depth: 0, 0), (trailing, lambda depth: height - depth, HALO - 1)):
        for plane in range(planes):
            for kind, depth in enumerate((HALO, HALO, HALO - 1)):
                start, place = (start_of(depth), plane * PACKED)
                value = plane_of(state, third, before, after, kind, plane, slice(start, start + depth))
                if value is None:
                    value = jnp.zeros((depth, width), jnp.float32)
                side[place + kind * HALO:place + kind * HALO + depth, :] = value
                if kind < 2:
                    edge = value[nearest:nearest + 1]
                    side[place + LAYERS + kind:place + LAYERS + kind + 1, :] = edge - rounded(edge)
        filled = planes * PACKED
        if filled < side.shape[0]:
            side[filled:, :] = jnp.zeros((side.shape[0] - filled, width), jnp.float32)
    leading_ref[...] = leading[...].astype(jnp.bfloat16)
    trailing_ref[...] = trailing[...].astype(jnp.bfloat16)


def strips_of(planes, width):
    each = width // (2 * HALO)
    places = {}
    for kind in range(3):
        for plane in range(kind // 2, planes - kind // 2):
            number = len(places)
            places[kind, plane] = (number // each, (number % each) * 2 * HALO)
    return places, -(-len(places) // each)


def assemble_body(state, third, before, after, below_ref, above_ref, whole_ref, strips_ref, below, above, strips):
    _, height, width = state.shape[1:]
    planes, rows = whole_ref.shape[1:3]
    places, count = strips_of(planes, width)
    lanes = lax.broadcasted_iota(jnp.int32, (rows, width), 1)
    below[...] = below_ref[...].astype(jnp.float32)
    above[...] = above_ref[...].astype(jnp.float32)
    tiles = {}

    def gather_lanes(tile, value, shift, first, size):
        turned = pltpu.roll(value, shift, axis=1)
        here = (lanes >= first) & (lanes < first + size)
        tiles[tile] = jnp.where(here, turned, tiles[tile]) if tile in tiles else turned

    for kind, depth in enumerate((HALO, HALO, HALO - 1)):
        for plane in range(planes):
            value = plane_of(state, third, before, after, kind, plane, slice(0, height))
            if value is None:
                continue
            held = slice(plane * PACKED + kind * HALO, plane * PACKED + kind * HALO + depth)
            whole_ref[kind, plane, EDGE:EDGE + height, :] = value
            whole_ref[kind, plane, EDGE - depth:EDGE, :] = below[held, :]
            whole_ref[kind, plane, EDGE + height:EDGE + height + depth, :] = above[held, :]
            if kind < 2:
                rest = slice(plane * PACKED + LAYERS + kind, plane * PACKED + LAYERS + kind + 1)
                whole_ref[kind, plane, EDGE - 1:EDGE, :] = below[held.stop - 1:held.stop, :] + below[rest, :]
                whole_ref[kind, plane, EDGE + height:EDGE + height + 1, :] = (
                    above[held.start:held.start + 1, :] + above[rest, :])
            tile, shift = places[kind, plane]
            value = whole_ref[kind, plane]
            gather_lanes(tile, value, (shift + HALO) % width, shift, 2 * HALO)
            if kind < 2:
                first = 2 * (kind * planes + plane)
                gather_lanes(count, value - rounded(value), first + 1, first, 2)
    for tile, value in tiles.items():
        strips[tile * rows:(tile + 1) * rows, :] = value
    filled = len(tiles) * rows
    if filled < strips.shape[0]:
        strips[filled:, :] = jnp.zeros((strips.shape[0] - filled, width), jnp.float32)
    strips_ref[...] = strips[...].astype(jnp.bfloat16)


def load_sides(whole, earlier, later, kind, target, first):
    planes, rows, width = whole.shape[1:]
    places, count = strips_of(planes, width)
    lanes = lax.broadcasted_iota(jnp.int32, (rows, width), 1)

    def both(tile, shift, size):
        held = slice(tile * rows, (tile + 1) * rows)
        after = (lanes >= shift + size) & (lanes < shift + 2 * size)
        return pltpu.roll(jnp.where(after, later[held, :], earlier[held, :]), (2 * width - shift - size) % width, axis=1)

    for plane in range(planes):
        if (kind, plane) not in places:
            continue
        value = both(*places[kind, plane], HALO)
        if kind < 2:
            rest = both(count, 2 * (kind * planes + plane), 1)
            value = value + jnp.where((lanes == 0) | (lanes == width - 1), rest, 0.0)
        target[plane, first:first + rows, :] = value


def one_step(source, target, fixed, planes, rows, sides):
    def some_rows(plane, first):
        held, here = (slice(8 + first, 16 + first), slice(first, first + 8))
        around, centers = ([], [])
        for pair in source:
            summed, center = ([], [])
            for field in pair:
                middle = field[plane, held, :]
                total = -6.0 * middle + field[plane + 1, held, :] + field[plane - 1, held, :]
                summed.append(total + field[plane, 9 + first:17 + first, :] + field[plane, 7 + first:15 + first, :])
                center.append(middle)
            width = center[0].shape[1]
            lanes = lax.broadcasted_iota(jnp.int32, center[0].shape, 1)
            up = [pltpu.roll(value, 1, axis=1) for value in center]
            down = [pltpu.roll(value, width - 1, axis=1) for value in center]
            around.append([summed[n] + jnp.where(lanes == 0, up[1 - n], up[n])
                           + jnp.where(lanes == width - 1, down[1 - n], down[n]) for n in range(2)])
            centers.append(center)
        for n in range(2 if sides else 1):
            still = [pair[n][plane, here, :] for pair in fixed] + [None]
            new = react(centers[0][n], centers[1][n], still[0], around[0][n], around[1][n], still[1])
            for pair, value in zip(target, new):
                pair[n][plane, held, :] = value

    def one_plane(plane, carry):
        for first in range(0, rows, 8):
            some_rows(plane, first)
        return carry

    lax.fori_loop(planes[0], planes[1], one_plane, 0, unroll=True)


def run_steps(whole, earlier, later, fixed, now, then):
    planes, rows = whole.shape[1:3]
    for kind, pair in enumerate(now):
        load_sides(whole, earlier, later, kind, pair[1], 8)
        for plane in range(planes):
            pair[0][plane, 8:8 + rows, :] = whole[kind, plane]
    for step in range(HALO):
        one_step(now, then, fixed, (step + 1, planes - step - 1), rows, step < HALO - 1)
        now, then = then, now
    return now[0][0], now[1][0]


def move_order(patches_z, edge):
    lanes = patches_z * edge
    row = lax.broadcasted_iota(jnp.int32, (lanes, lanes), 0)
    column = lax.broadcasted_iota(jnp.int32, (lanes, lanes), 1)
    return jnp.where((row % patches_z) * edge + row // patches_z == column, 1.0, 0.0).astype(jnp.bfloat16)


def cell_order(edge):
    cells = edge ** 3
    row = lax.broadcasted_iota(jnp.int32, (cells, cells), 0)
    column = lax.broadcasted_iota(jnp.int32, (cells, cells), 1)
    return jnp.where((row % (edge * edge)) * edge + row // (edge * edge) == column, 1.0, 0.0).astype(jnp.bfloat16)


def half_tiles(source, count, rows, by_lane):
    half = by_lane // 2
    lanes = lax.broadcasted_iota(jnp.int32, (rows, by_lane), 1)
    out = []
    for b in range(count[1]):
        tiles = []
        for a in range(0, count[0], 2):
            low, high = [source[n * rows:(n + 1) * rows, (b // 2) * by_lane:(b // 2 + 1) * by_lane] for n in (a, a + 1)]
            if b % 2 == 0:
                high = pltpu.roll(high, half, axis=1)
            else:
                low = pltpu.roll(low, half, axis=1)
            tiles.append(jnp.where(lanes < half, low, high))
        out.append(jnp.concatenate(tiles, axis=1))
    return jnp.concatenate(out, axis=0)


def cube_starts(shape, edge):
    extent_x, extent_y = shape
    return [(px * edge + ix, py * edge) for px in range(extent_x // edge) for py in range(extent_y // edge)
            for ix in range(edge)]


def exact_product(left, right):
    high = left.astype(jnp.bfloat16)
    low = (left - high.astype(jnp.float32)).astype(jnp.bfloat16)
    return product(high, right) + product(low, right)


def paired(refs):
    pairs = list(zip(refs[::2], refs[1::2]))
    return pairs[:2], pairs[2:]


def first_steps_body(edge, whole, earlier_ref, later_ref, state_ref, inputs_ref, targets_ref, fixed_ref, *scratch):
    *fields_now, side, earlier, later, column_ref, semaphores = scratch
    length, height, width = state_ref.shape[1:]
    earlier[...] = earlier_ref[...].astype(jnp.float32)
    later[...] = later_ref[...].astype(jnp.float32)
    load_sides(whole, earlier, later, 2, side, 0)
    copies = start_copies([(whole.at[2], fixed_ref.at[0]), (side, fixed_ref.at[1])], semaphores)
    now = run_steps(whole, earlier, later, [(whole.at[2], side)], *paired(fields_now))
    move, order = (move_order(width // edge, edge), cell_order(edge))
    for species, (field, out_ref) in enumerate(zip(now, (inputs_ref, targets_ref))):
        for x in range(length):
            state_ref[species, x] = field[x + HALO, 8 + EDGE:8 + EDGE + height, :]
        for number, (x, y) in enumerate(cube_starts((length, height), edge)):
            column_ref[number * edge:(number + 1) * edge, :] = state_ref[species, x, y:y + edge, :]
        turned = product_transposed(move, column_ref[...].astype(jnp.bfloat16))
        columns = length * height // (edge * edge)
        cubes = half_tiles(turned, (edge, columns), width // edge, 2 * edge * edge)
        out_ref[...] = product(cubes.astype(jnp.bfloat16), order).astype(jnp.bfloat16)
    for copy in copies:
        copy.wait()


def own_forward_body(edge, inputs_ref, first_ref, middle_ref, last_ref, field_ref):
    length, height, width = field_ref.shape
    h1 = gelu_value(product(inputs_ref[...], first_ref[...])).astype(jnp.bfloat16)
    h2 = gelu_value(product(h1, middle_ref[...])).astype(jnp.bfloat16)
    forcing = product(h2, last_ref[...])
    cells = lax.broadcasted_iota(jnp.int32, (edge ** 3, edge ** 3), 1)
    row = lax.broadcasted_iota(jnp.int32, (edge ** 3, edge ** 3), 0)
    square = edge * edge
    order = jnp.where((cells % square) * edge + cells // square == row, 1.0, 0.0).astype(jnp.bfloat16)
    columns = length * height // square
    turned = half_tiles(exact_product(forcing, order), (columns, edge), width // edge, 2 * square)
    moved = exact_product(turned.T, move_order(width // edge, edge))
    for number, (x, y) in enumerate(cube_starts((length, height), edge)):
        field_ref[x, y:y + edge, :] = moved[number * edge:(number + 1) * edge, :]


def last_steps_body(whole, earlier_ref, later_ref, fixed, state_ref, *scratch):
    *fields_now, side, earlier, later = scratch
    length, height, _ = state_ref.shape[1:]
    earlier[...] = earlier_ref[...].astype(jnp.float32)
    later[...] = later_ref[...].astype(jnp.float32)
    load_sides(whole, earlier, later, 2, side, 0)
    both = [(fixed.at[0], fixed.at[1]), (whole.at[2], side)]
    now = run_steps(whole, earlier, later, both, *paired(fields_now))
    for species, field in enumerate(now):
        for x in range(length):
            state_ref[species, x] = field[x + HALO, 8 + EDGE:8 + EDGE + height, :]


def start_copies(pairs, semaphores):
    copies = [pltpu.make_async_copy(*pair, semaphores.at[number]) for number, pair in enumerate(pairs)]
    for copy in copies:
        copy.start()
    return copies


def bring_body(far_ref, near_ref, semaphores):
    start_copies([(far_ref, near_ref)], semaphores)[0].wait()


def store_faces(state, third, leading_ref, trailing_ref):
    length = third.shape[0]
    for kind, depth in enumerate((HALO, HALO, HALO - 1)):
        read = fields(state, third)[kind][0]
        for plane in range(depth):
            for out_ref, x, nearest in ((leading_ref, plane, 0), (trailing_ref, length - depth + plane, length - 1)):
                value = read(x, slice(None))
                out_ref[kind * HALO + plane] = value.astype(jnp.bfloat16)
                if kind < 2 and x == nearest:
                    out_ref[LAYERS + kind] = (value - rounded(value)).astype(jnp.bfloat16)


def first_faces_body(state_ref, third_ref, leading_ref, trailing_ref, state_out, third_out, semaphores):
    for copy in start_copies(((state_ref, state_out), (third_ref, third_out)), semaphores):
        copy.wait()
    store_faces(state_out, third_out, leading_ref, trailing_ref)


def x_halos(leading, trailing):
    return ring(trailing, "gx", 1), ring(leading, "gx", -1)


def edge_rows(state, third, before, after):
    planes = state.shape[1] + 2 * HALO
    packed = (whole_tiles(planes * PACKED), state.shape[3])
    return kernel_call(edge_rows_body, [(packed, jnp.bfloat16)] * 2, scratch=[(packed, jnp.float32)] * 2)(
        state, third, before, after
    )


def y_halos(leading, trailing):
    return ring(trailing, "gy", 1), ring(leading, "gy", -1)


def assemble(state, third, before, after, below, above):
    length, height, width = state.shape[1:]
    planes, rows = (length + 2 * HALO, height + 2 * EDGE)
    strips = (whole_tiles((strips_of(planes, width)[1] + 1) * rows), width)
    outputs = [((3, planes, rows, width), jnp.float32), (strips, jnp.bfloat16)]
    scratch = [(shape, jnp.float32) for shape in (below.shape, above.shape, strips)]
    return kernel_call(assemble_body, outputs, scratch=scratch)(
        state, third, before, after, below, above
    )


def z_strips(strips):
    earlier = ring(strips, "row", 1)
    return earlier, (earlier if lax.axis_size("row") == 2 else ring(strips, "row", -1))


def exchange(array, mesh_sizes, flips):
    size_x, size_y, size_r = mesh_sizes
    route = []
    for i in range(size_x):
        for j in range(size_y):
            for k in range(size_r):
                here = (i * size_y + j) * size_r + k
                there = ((i ^ flips[0]) * size_y + (j ^ flips[1])) * size_r + (k ^ flips[2])
                route.append((here, there))
    return lax.ppermute(array, ("gx", "gy", "row"), route)


def reduction_stages(mesh_sizes):
    size_x, size_y, _ = mesh_sizes
    stages = []
    bit = 1
    while bit < size_x:
        stages.append((bit, 0, 0))
        bit *= 2
    bit = 2
    while bit < size_y:
        stages.append((0, bit, 0))
        bit *= 2
    return stages


def chosen_rows(total, mesh_sizes):
    size_x, size_y, size_r = mesh_sizes
    stages = reduction_stages(mesh_sizes)
    unit = total // (size_x * size_y * size_r)
    blocks = 1 << len(stages)
    position = jnp.arange(blocks * unit, dtype=jnp.int32)
    place, inner = (position // unit, position % unit)
    x = jnp.zeros_like(position) + lax.axis_index("gx")
    y = jnp.zeros_like(position) + lax.axis_index("gy")
    for number, (bit_x, bit_y, _) in enumerate(stages):
        leaves = 1 - (place >> (len(stages) - 1 - number)) % 2
        x = x ^ (leaves * bit_x)
        y = y ^ (leaves * bit_y)
    block = (x * size_y + y) * size_r + lax.axis_index("row")
    return (block * unit + inner)[:, None]


def halved(leaving, staying, flips, mesh_sizes):
    arrived = exchange(leaving, mesh_sizes, flips)
    half = staying.shape[0] // 2
    return staying[:half] + arrived[:half], staying[half:] + arrived[half:]


def rest_halved(leaving, staying, stages, done, mesh_sizes):
    for number in range(done, len(stages) - 1):
        leaving, staying = halved(leaving, staying, stages[number], mesh_sizes)
    arrived = exchange(leaving, mesh_sizes, stages[-1])
    return staying + arrived


def gelu_pair(values):
    root = math.sqrt(2.0 / math.pi)
    square = values * values
    bend = jnp.tanh(values * (root + (root * 0.044715) * square))
    cdf = 0.5 + 0.5 * bend
    slope = cdf + (0.5 * values) * (1.0 - bend * bend) * (root + (3.0 * root * 0.044715) * square)
    return values * cdf, slope


def gelu_value(values):
    root = math.sqrt(2.0 / math.pi)
    return values * (0.5 + 0.5 * jnp.tanh(values * (root + (root * 0.044715) * (values * values))))


def product(left, right):
    return jnp.dot(left, right, preferred_element_type=jnp.float32)


def product_transposed(left, right):
    return lax.dot_general(left, right, (((1,), (1,)), ((), ())), preferred_element_type=jnp.float32)


def transposed_choice(rows, source):
    columns = lax.broadcasted_iota(jnp.int32, (rows.shape[0], source.shape[1]), 1)
    choice = jnp.where(columns == rows, 1.0, 0.0).astype(jnp.bfloat16)
    return product_transposed(choice, source).astype(jnp.bfloat16)


def column_tiles(width):
    tile = 256 if width % 256 == 0 else width
    return [slice(start, start + tile) for start in range(0, width, tile)]


def store_halves(value, columns, leaving_ref, staying_ref):
    half = value.shape[0] // 2
    leaving_ref[:, columns] = value[:half]
    staying_ref[:, columns] = value[half:]


def activated(left, weight, value_ref, slope_ref):
    tiles = column_tiles(value_ref.shape[1])
    ahead = product(left, weight[:, tiles[0]])
    for number, columns in enumerate(tiles):
        now = ahead
        if number + 1 < len(tiles):
            ahead = product(left, weight[:, tiles[number + 1]])
        value, slope = gelu_pair(now)
        value_ref[:, columns] = value.astype(jnp.bfloat16)
        slope_ref[:, columns] = slope


def forward_one_body(own_ref, a_ref, b_ref, c_ref, first_ref, middle_ref,
                     x_ref, h1_ref, s1_ref, h2_ref, s2_ref):
    count = own_ref.shape[0]
    for number, part in enumerate((own_ref, a_ref, b_ref, c_ref)):
        x_ref[number * count:(number + 1) * count, :] = part[...]
    activated(x_ref[...], first_ref, h1_ref, s1_ref)
    activated(h1_ref[...], middle_ref, h2_ref, s2_ref)


def forward_two_body(scale, h2_ref, own_ref, a_ref, b_ref, c_ref, last_ref, rows_ref, error_ref, leaving_ref, staying_ref):
    count = own_ref.shape[0]
    h2 = h2_ref[...]
    for columns in column_tiles(error_ref.shape[1]):
        forcing = product(h2, last_ref[:, columns])
        for number, part in enumerate((own_ref, a_ref, b_ref, c_ref)):
            block = slice(number * count, (number + 1) * count)
            target = part[:, columns].astype(jnp.float32)
            error_ref[block, columns] = ((forcing[block] - target) * scale).astype(jnp.bfloat16)
    chosen = transposed_choice(rows_ref[...], h2)
    for columns in column_tiles(error_ref.shape[1]):
        store_halves(product(chosen, error_ref[:, columns]), columns, leaving_ref, staying_ref)


def backward_body(carried_ref, weight_ref, slope_ref, source_ref, rows_ref, back_ref, leaving_ref, staying_ref):
    carried = carried_ref[...]
    for columns in column_tiles(back_ref.shape[1]):
        value = product_transposed(carried, weight_ref[columns, :]) * slope_ref[:, columns]
        back_ref[:, columns] = value.astype(jnp.bfloat16)
    chosen = transposed_choice(rows_ref[...], source_ref[...])
    for columns in column_tiles(back_ref.shape[1]):
        store_halves(product(chosen, back_ref[:, columns]), columns, leaving_ref, staying_ref)


def tied(value, *others):
    return lax.optimization_barrier((value, *others))[0]


def kernel_call(body, outputs, scratch=(), flops=1 << 31, far=(), far_outputs=(), copies=0):
    def call(*inputs):
        near, away = (pl.BlockSpec(memory_space=pltpu.VMEM), pl.BlockSpec(memory_space=pltpu.HBM))
        result = pl.pallas_call(
            body,
            cost_estimate=pl.CostEstimate(flops=flops, transcendentals=0, bytes_accessed=0),
            in_specs=[away if number in far else near for number in range(len(inputs))],
            out_specs=[away if number in far_outputs else near for number in range(len(outputs))],
            out_shape=[(pltpu.HBM if number in far_outputs else jax.ShapeDtypeStruct)(shape, dtype)
                       for number, (shape, dtype) in enumerate(outputs)],
            scratch_shapes=[pltpu.VMEM(shape, dtype) for shape, dtype in scratch]
            + [pltpu.SemaphoreType.DMA((copies,))] * (copies > 0),
            compiler_params=pltpu.CompilerParams(vmem_limit_bytes=VMEM_LIMIT),
        )(*(pltpu.with_memory_space_constraint(array, pltpu.HBM) if number in far else array
            for number, array in enumerate(inputs)))
        return result

    return call


def all_steps(concentrations, diffusivity, weight_first, weight_middle, weight_last):
    mesh_sizes = tuple(lax.axis_size(axis) for axis in ("gx", "gy", "row"))
    length, height, width = diffusivity.shape
    f32, bf16 = (jnp.float32, jnp.bfloat16)
    planes, rows = (length + 2 * HALO, height + 2 * EDGE)
    fixed = ((2, planes, rows, width), f32)
    buffers = [((planes, 8 + rows + 8, width), f32)] * 8 + [((planes, rows, width), f32)]
    buffers += [((whole_tiles((strips_of(planes, width)[1] + 1) * rows), width), f32)] * 2
    count = length * height * width // PATCH ** 3
    cells, hidden = weight_first.shape
    hidden_second = weight_middle.shape[1]
    total = 4 * count
    rows_first, rows_middle, rows_last = [chosen_rows(size, mesh_sizes) for size in (cells, hidden, hidden_second)]
    half_of = lambda chosen, width: ((chosen.shape[0] // 2, width), f32)
    stages = reduction_stages(mesh_sizes)
    big = 1 << 32

    layers = ((PACKED, height, width), bf16)
    leading, trailing, near_state, near_third = kernel_call(
        first_faces_body, [layers, layers, (concentrations.shape, f32), (diffusivity.shape, f32)],
        far=(0, 1), copies=2,
    )(concentrations, diffusivity)
    before, after = x_halos(leading, trailing)
    (near_last,) = kernel_call(bring_body, [(weight_last.shape, bf16)], far=(0,), copies=1)(weight_last)
    leading, trailing = edge_rows(near_state, near_third, before, after)
    below, above = y_halos(leading, trailing)
    whole, strips = assemble(near_state, near_third, before, after, below, above)
    state, inputs, targets, diffusivity_fixed = kernel_call(
        functools.partial(first_steps_body, PATCH),
        [(concentrations.shape, f32), ((count, cells), bf16), ((count, cells), bf16), fixed],
        scratch=buffers + [((length * height, width), f32)],
        far_outputs=(3,), copies=2,
    )(whole, *z_strips(strips))

    gather = lambda array: [exchange(array, mesh_sizes, flips) for flips in ((0, 0, 1), (0, 1, 0), (0, 1, 1))]
    all_inputs = gather(inputs)
    (field,) = kernel_call(functools.partial(own_forward_body, PATCH), [(diffusivity.shape, f32)],
        flops=big // 4,
    )(
        inputs, weight_first, weight_middle, near_last
    )
    all_targets = gather(tied(targets, field))
    leading, trailing = kernel_call(store_faces, [layers, layers])(state, field)
    before, after = x_halos(leading, trailing)
    x, h1, s1, h2, s2 = kernel_call(
        forward_one_body,
        [((total, cells), bf16), ((total, hidden), bf16), ((total, hidden), f32), ((total, hidden_second), bf16),
         ((total, hidden_second), f32)],
        flops=big,
    )(tied(inputs, leading, trailing), *all_inputs, weight_first, weight_middle)
    leading, trailing = edge_rows(state, field, tied(before, h2), after)
    below, above = y_halos(leading, trailing)
    error, *last = kernel_call(
        functools.partial(forward_two_body, 1.0 / count),
        [((total, cells), bf16), half_of(rows_last, cells), half_of(rows_last, cells)],
        flops=big,
    )(tied(h2, leading, trailing), targets, *all_targets, weight_last, rows_last)
    last = halved(*last, stages[0], mesh_sizes)
    back_second, *middle = kernel_call(
        backward_body,
        [((total, hidden_second), bf16), half_of(rows_middle, hidden_second), half_of(rows_middle, hidden_second)],
        flops=big // 2,
    )(error, weight_last, s2, h1, rows_middle)
    middle = halved(*middle, stages[0], mesh_sizes)
    last_leaving = last[0]
    whole, strips = assemble(state, field, before, after, tied(below, back_second, last_leaving, middle[0]), above)
    last = halved(*last, stages[1], mesh_sizes)
    back_first, *first = kernel_call(
        backward_body,
        [((total, hidden), bf16), half_of(rows_first, hidden), half_of(rows_first, hidden)],
        flops=big // 2,
    )(tied(back_second, strips), weight_middle, s1, x, rows_first)
    first = halved(*first, stages[0], mesh_sizes)
    middle = halved(*middle, stages[1], mesh_sizes)
    (state,) = kernel_call(last_steps_body, [(state.shape, f32)], scratch=buffers, flops=big)(
        tied(whole, first[0], middle[0], last[0]), *z_strips(strips), diffusivity_fixed
    )
    grads = [rest_halved(*part, stages, done, mesh_sizes) for part, done in ((first, 1), (middle, 2), (last, 2))]
    return (state, *grads)


def solution(mesh):
    in_specs = (P(None, "gx", "gy", "row"), P("gx", "gy", "row"), P(), P(), P())
    out_specs = (
        P(None, "gx", "gy", "row"),
        P(("gx", "gy", "row"), None),
        P(("gx", "gy", "row"), None),
        P(("gx", "gy", "row"), None),
    )
    return jax.shard_map(all_steps, mesh=mesh, in_specs=in_specs, out_specs=out_specs, check_vma=False)
```

```python
import functools
import math

import jax
import jax.numpy as jnp
from jax import lax
from jax.experimental import pallas as pl
from jax.experimental.pallas import tpu as pltpu
from jax.sharding import PartitionSpec as P

STEPS = 6
PATCH = 8
HALO = STEPS // 2
EDGE = 4
VMEM_LIMIT = 20 << 20


def ring(array, axis, distance):
    size = lax.axis_size(axis)
    return lax.ppermute(array, axis, [(i, (i + distance) % size) for i in range(size)])


def react(activator, inhibitor, diffusivity, lap_activator, lap_inhibitor, forcing):
    product = activator * inhibitor * inhibitor
    inner = diffusivity * lap_activator - product + 0.04 * (1.0 - activator)
    new_activator = activator + 0.1 * (inner if forcing is None else inner + forcing)
    new_inhibitor = inhibitor + 0.1 * (
        0.5 * diffusivity * lap_inhibitor + product - 0.1 * inhibitor
    )
    return (new_activator, new_inhibitor)


def fields(state, third):
    return ((lambda x, rows: state[0, x, rows, :], HALO), (lambda x, rows: state[1, x, rows, :], HALO),
            (lambda x, rows: third[x, rows, :], HALO - 1))


LAYERS = 3 * HALO - 1
PACKED = LAYERS + 2


def rounded(value):
    return value.astype(jnp.bfloat16).astype(jnp.float32)


def whole_tiles(rows):
    return -(-rows // 16) * 16


def plane_of(state, third, before, after, kind, plane, rows):
    read, depth = fields(state, third)[kind]
    length = state.shape[1]
    x = plane - HALO
    if x < -depth or x >= length + depth:
        return None
    if 0 <= x < length:
        return read(x, rows)
    halo, layer = (before, kind * HALO + depth + x) if x < 0 else (after, kind * HALO + x - length)
    value = halo[layer].astype(jnp.float32)
    if kind < 2 and x in (-1, length):
        value = value + halo[LAYERS + kind].astype(jnp.float32)
    return value[rows]


def edge_rows_body(state, third, before, after, leading_ref, trailing_ref, leading, trailing):
    length, height, width = state.shape[1:]
    planes = length + 2 * HALO
    for side, start_of, nearest in ((leading, lambda depth: 0, 0), (trailing, lambda depth: height - depth, HALO - 1)):
        for plane in range(planes):
            for kind, depth in enumerate((HALO, HALO, HALO - 1)):
                start, place = (start_of(depth), plane * PACKED)
                value = plane_of(state, third, before, after, kind, plane, slice(start, start + depth))
                if value is None:
                    value = jnp.zeros((depth, width), jnp.float32)
                side[place + kind * HALO:place + kind * HALO + depth, :] = value
                if kind < 2:
                    edge = value[nearest:nearest + 1]
                    side[place + LAYERS + kind:place + LAYERS + kind + 1, :] = edge - rounded(edge)
        filled = planes * PACKED
        if filled < side.shape[0]:
            side[filled:, :] = jnp.zeros((side.shape[0] - filled, width), jnp.float32)
    leading_ref[...] = leading[...].astype(jnp.bfloat16)
    trailing_ref[...] = trailing[...].astype(jnp.bfloat16)


def strips_of(planes, width):
    each = width // (2 * HALO)
    places = {}
    for kind in range(3):
        for plane in range(kind // 2, planes - kind // 2):
            number = len(places)
            places[kind, plane] = (number // each, (number % each) * 2 * HALO)
    return places, -(-len(places) // each)


def assemble_body(state, third, before, after, below_ref, above_ref, whole_ref, strips_ref, below, above, strips):
    _, height, width = state.shape[1:]
    planes, rows = whole_ref.shape[1:3]
    places, count = strips_of(planes, width)
    lanes = lax.broadcasted_iota(jnp.int32, (rows, width), 1)
    below[...] = below_ref[...].astype(jnp.float32)
    above[...] = above_ref[...].astype(jnp.float32)
    tiles = {}

    def gather_lanes(tile, value, shift, first, size):
        turned = pltpu.roll(value, shift, axis=1)
        here = (lanes >= first) & (lanes < first + size)
        tiles[tile] = jnp.where(here, turned, tiles[tile]) if tile in tiles else turned

    for kind, depth in enumerate((HALO, HALO, HALO - 1)):
        for plane in range(planes):
            value = plane_of(state, third, before, after, kind, plane, slice(0, height))
            if value is None:
                continue
            held = slice(plane * PACKED + kind * HALO, plane * PACKED + kind * HALO + depth)
            whole_ref[kind, plane, EDGE:EDGE + height, :] = value
            whole_ref[kind, plane, EDGE - depth:EDGE, :] = below[held, :]
            whole_ref[kind, plane, EDGE + height:EDGE + height + depth, :] = above[held, :]
            if kind < 2:
                rest = slice(plane * PACKED + LAYERS + kind, plane * PACKED + LAYERS + kind + 1)
                whole_ref[kind, plane, EDGE - 1:EDGE, :] = below[held.stop - 1:held.stop, :] + below[rest, :]
                whole_ref[kind, plane, EDGE + height:EDGE + height + 1, :] = (
                    above[held.start:held.start + 1, :] + above[rest, :])
            tile, shift = places[kind, plane]
            value = whole_ref[kind, plane]
            gather_lanes(tile, value, (shift + HALO) % width, shift, 2 * HALO)
            if kind < 2:
                first = 2 * (kind * planes + plane)
                gather_lanes(count, value - rounded(value), first + 1, first, 2)
    for tile, value in tiles.items():
        strips[tile * rows:(tile + 1) * rows, :] = value
    filled = len(tiles) * rows
    if filled < strips.shape[0]:
        strips[filled:, :] = jnp.zeros((strips.shape[0] - filled, width), jnp.float32)
    strips_ref[...] = strips[...].astype(jnp.bfloat16)


def load_sides(whole, earlier, later, kind, target, first):
    planes, rows, width = whole.shape[1:]
    places, count = strips_of(planes, width)
    lanes = lax.broadcasted_iota(jnp.int32, (rows, width), 1)

    def both(tile, shift, size):
        held = slice(tile * rows, (tile + 1) * rows)
        after = (lanes >= shift + size) & (lanes < shift + 2 * size)
        return pltpu.roll(jnp.where(after, later[held, :], earlier[held, :]), (2 * width - shift - size) % width, axis=1)

    for plane in range(planes):
        if (kind, plane) not in places:
            continue
        value = both(*places[kind, plane], HALO)
        if kind < 2:
            rest = both(count, 2 * (kind * planes + plane), 1)
            value = value + jnp.where((lanes == 0) | (lanes == width - 1), rest, 0.0)
        target[plane, first:first + rows, :] = value


def one_step(source, target, fixed, planes, rows, sides, finished=None):
    def some_rows(plane, first):
        held, here = (slice(8 + first, 16 + first), slice(first, first + 8))
        around, centers = ([], [])
        for pair in source:
            summed, center = ([], [])
            for field in pair:
                middle = field[plane, held, :]
                total = -6.0 * middle + field[plane + 1, held, :] + field[plane - 1, held, :]
                summed.append(total + field[plane, 9 + first:17 + first, :] + field[plane, 7 + first:15 + first, :])
                center.append(middle)
            width = center[0].shape[1]
            lanes = lax.broadcasted_iota(jnp.int32, center[0].shape, 1)
            up = [pltpu.roll(value, 1, axis=1) for value in center]
            down = [pltpu.roll(value, width - 1, axis=1) for value in center]
            around.append([summed[n] + jnp.where(lanes == 0, up[1 - n], up[n])
                           + jnp.where(lanes == width - 1, down[1 - n], down[n]) for n in range(2)])
            centers.append(center)
        for n in range(2 if sides else 1):
            still = [pair[n][plane, here, :] for pair in fixed] + [None]
            new = react(centers[0][n], centers[1][n], still[0], around[0][n], around[1][n], still[1])
            for pair, value in zip(target, new):
                pair[n][plane, held, :] = value

    for plane in range(*planes):
        for first in range(0, rows, 8):
            some_rows(plane, first)
        if finished is not None:
            finished(plane, target)


def run_steps(whole, earlier, later, fixed, now, then, finished=None):
    planes, rows = whole.shape[1:3]
    for kind, pair in enumerate(now):
        load_sides(whole, earlier, later, kind, pair[1], 8)
        for plane in range(planes):
            pair[0][plane, 8:8 + rows, :] = whole[kind, plane]
    for step in range(HALO):
        one_step(now, then, fixed, (step + 1, planes - step - 1), rows, step < HALO - 1, finished if step == HALO - 1 else None)
        now, then = then, now
    return now[0][0], now[1][0]


def move_order(patches_z, edge):
    lanes = patches_z * edge
    row = lax.broadcasted_iota(jnp.int32, (lanes, lanes), 0)
    column = lax.broadcasted_iota(jnp.int32, (lanes, lanes), 1)
    return jnp.where((row % patches_z) * edge + row // patches_z == column, 1.0, 0.0).astype(jnp.bfloat16)


def cell_order(edge):
    cells = edge ** 3
    row = lax.broadcasted_iota(jnp.int32, (cells, cells), 0)
    column = lax.broadcasted_iota(jnp.int32, (cells, cells), 1)
    return jnp.where((row % (edge * edge)) * edge + row // (edge * edge) == column, 1.0, 0.0).astype(jnp.bfloat16)


def half_tiles(source, count, rows, by_lane):
    half = by_lane // 2
    lanes = lax.broadcasted_iota(jnp.int32, (rows, by_lane), 1)
    out = []
    for b in range(count[1]):
        tiles = []
        for a in range(0, count[0], 2):
            low, high = [source[n * rows:(n + 1) * rows, (b // 2) * by_lane:(b // 2 + 1) * by_lane] for n in (a, a + 1)]
            if b % 2 == 0:
                high = pltpu.roll(high, half, axis=1)
            else:
                low = pltpu.roll(low, half, axis=1)
            tiles.append(jnp.where(lanes < half, low, high))
        out.append(jnp.concatenate(tiles, axis=1))
    return jnp.concatenate(out, axis=0)


def cube_starts(shape, edge):
    extent_x, extent_y = shape
    return [(px * edge + ix, py * edge) for px in range(extent_x // edge) for py in range(extent_y // edge)
            for ix in range(edge)]


def exact_product(left, right):
    high = left.astype(jnp.bfloat16)
    low = (left - high.astype(jnp.float32)).astype(jnp.bfloat16)
    return product(high, right) + product(low, right)


def paired(refs):
    pairs = list(zip(refs[::2], refs[1::2]))
    return pairs[:2], pairs[2:]


def first_steps_body(edge, whole, earlier_ref, later_ref, state_ref, inputs_ref, targets_ref, fixed_ref, *scratch):
    *fields_now, side, earlier, later, column_ref, semaphores = scratch
    length, height, width = state_ref.shape[1:]
    earlier[...] = earlier_ref[...].astype(jnp.float32)
    later[...] = later_ref[...].astype(jnp.float32)
    load_sides(whole, earlier, later, 2, side, 0)
    copies = start_copies([(whole.at[2], fixed_ref.at[0]), (side, fixed_ref.at[1])], semaphores)
    now = run_steps(whole, earlier, later, [(whole.at[2], side)], *paired(fields_now))
    move, order = (move_order(width // edge, edge), cell_order(edge))
    for species, (field, out_ref) in enumerate(zip(now, (inputs_ref, targets_ref))):
        for x in range(length):
            state_ref[species, x] = field[x + HALO, 8 + EDGE:8 + EDGE + height, :]
        for number, (x, y) in enumerate(cube_starts((length, height), edge)):
            column_ref[number * edge:(number + 1) * edge, :] = state_ref[species, x, y:y + edge, :]
        turned = product_transposed(move, column_ref[...].astype(jnp.bfloat16))
        columns = length * height // (edge * edge)
        cubes = half_tiles(turned, (edge, columns), width // edge, 2 * edge * edge)
        out_ref[...] = product(cubes.astype(jnp.bfloat16), order).astype(jnp.bfloat16)
    for copy in copies:
        copy.wait()


def own_forward_body(edge, scale, inputs_ref, targets_ref, first_ref, middle_ref, last_ref, field_ref, error_ref):
    length, height, width = field_ref.shape
    h1 = gelu_value(product(inputs_ref[...], first_ref[...])).astype(jnp.bfloat16)
    h2 = gelu_value(product(h1, middle_ref[...])).astype(jnp.bfloat16)
    forcing = product(h2, last_ref[...])
    error_ref[...] = ((forcing - targets_ref[...].astype(jnp.float32)) * scale).astype(jnp.bfloat16)
    cells = lax.broadcasted_iota(jnp.int32, (edge ** 3, edge ** 3), 1)
    row = lax.broadcasted_iota(jnp.int32, (edge ** 3, edge ** 3), 0)
    square = edge * edge
    order = jnp.where((cells % square) * edge + cells // square == row, 1.0, 0.0).astype(jnp.bfloat16)
    columns = length * height // square
    turned = half_tiles(exact_product(forcing, order), (columns, edge), width // edge, 2 * square)
    moved = exact_product(turned.T, move_order(width // edge, edge))
    for number, (x, y) in enumerate(cube_starts((length, height), edge)):
        field_ref[x, y:y + edge, :] = moved[number * edge:(number + 1) * edge, :]


def last_steps_body(whole, earlier_ref, later_ref, fixed, state_ref, *scratch):
    *fields_now, side, earlier, later, near, semaphores = scratch
    length, height, _ = state_ref.shape[1:]
    group = length // semaphores.shape[0]
    copies = []

    def finished(plane, pairs):
        x = plane - HALO
        for species, pair in enumerate(pairs):
            near[species, x] = pair[0][plane, 8 + EDGE:8 + EDGE + height, :]
        if (x + 1) % group == 0:
            held = slice(x + 1 - group, x + 1)
            copies.append(pltpu.make_async_copy(near.at[:, held], state_ref.at[:, held], semaphores.at[x // group]))
            copies[-1].start()

    earlier[...] = earlier_ref[...].astype(jnp.float32)
    later[...] = later_ref[...].astype(jnp.float32)
    load_sides(whole, earlier, later, 2, side, 0)
    both = [(fixed.at[0], fixed.at[1]), (whole.at[2], side)]
    run_steps(whole, earlier, later, both, *paired(fields_now), finished)
    for copy in copies:
        copy.wait()


def start_copies(pairs, semaphores):
    copies = [pltpu.make_async_copy(*pair, semaphores.at[number]) for number, pair in enumerate(pairs)]
    for copy in copies:
        copy.start()
    return copies


def bring_body(*refs):
    count = len(refs) // 2
    for copy in start_copies(zip(refs[:count], refs[count:-1]), refs[-1]):
        copy.wait()


def store_faces(state, third, leading_ref, trailing_ref):
    length = third.shape[0]
    for kind, depth in enumerate((HALO, HALO, HALO - 1)):
        read = fields(state, third)[kind][0]
        for plane in range(depth):
            for out_ref, x, nearest in ((leading_ref, plane, 0), (trailing_ref, length - depth + plane, length - 1)):
                value = read(x, slice(None))
                out_ref[kind * HALO + plane] = value.astype(jnp.bfloat16)
                if kind < 2 and x == nearest:
                    out_ref[LAYERS + kind] = (value - rounded(value)).astype(jnp.bfloat16)


def first_faces_body(state_ref, third_ref, leading_ref, trailing_ref, low, high, low_third, high_third, semaphores):
    length = third_ref.shape[0]
    for copy in start_copies((
        (state_ref.at[:, :HALO], low), (state_ref.at[:, length - HALO:], high),
        (third_ref.at[:HALO - 1], low_third), (third_ref.at[length - HALO + 1:], high_third),
    ), semaphores):
        copy.wait()
    for kind, depth in enumerate((HALO, HALO, HALO - 1)):
        for out_ref, near, third, nearest in ((leading_ref, low, low_third, 0), (trailing_ref, high, high_third, depth - 1)):
            for plane in range(depth):
                value = near[kind, plane] if kind < 2 else third[plane]
                out_ref[kind * HALO + plane] = value.astype(jnp.bfloat16)
                if kind < 2 and plane == nearest:
                    out_ref[LAYERS + kind] = (value - rounded(value)).astype(jnp.bfloat16)


def x_halos(leading, trailing):
    return ring(trailing, "gx", 1), ring(leading, "gx", -1)


def edge_rows(state, third, before, after):
    planes = state.shape[1] + 2 * HALO
    packed = (whole_tiles(planes * PACKED), state.shape[3])
    return kernel_call(edge_rows_body, [(packed, jnp.bfloat16)] * 2, scratch=[(packed, jnp.float32)] * 2)(
        state, third, before, after
    )


def y_halos(leading, trailing):
    return ring(trailing, "gy", 1), ring(leading, "gy", -1)


def assemble(state, third, before, after, below, above):
    length, height, width = state.shape[1:]
    planes, rows = (length + 2 * HALO, height + 2 * EDGE)
    strips = (whole_tiles((strips_of(planes, width)[1] + 1) * rows), width)
    outputs = [((3, planes, rows, width), jnp.float32), (strips, jnp.bfloat16)]
    scratch = [(shape, jnp.float32) for shape in (below.shape, above.shape, strips)]
    return kernel_call(assemble_body, outputs, scratch=scratch)(
        state, third, before, after, below, above
    )


def z_strips(strips):
    earlier = ring(strips, "row", 1)
    return earlier, (earlier if lax.axis_size("row") == 2 else ring(strips, "row", -1))


def exchange(array, mesh_sizes, flips):
    size_x, size_y, size_r = mesh_sizes
    route = []
    for i in range(size_x):
        for j in range(size_y):
            for k in range(size_r):
                here = (i * size_y + j) * size_r + k
                there = ((i ^ flips[0]) * size_y + (j ^ flips[1])) * size_r + (k ^ flips[2])
                route.append((here, there))
    return lax.ppermute(array, ("gx", "gy", "row"), route)


def reduction_stages(mesh_sizes):
    size_x, size_y, _ = mesh_sizes
    stages = []
    bit = 1
    while bit < size_x:
        stages.append((bit, 0, 0))
        bit *= 2
    bit = 2
    while bit < size_y:
        stages.append((0, bit, 0))
        bit *= 2
    return stages


def chosen_rows(total, mesh_sizes):
    size_x, size_y, size_r = mesh_sizes
    stages = reduction_stages(mesh_sizes)
    unit = total // (size_x * size_y * size_r)
    blocks = 1 << len(stages)
    position = jnp.arange(blocks * unit, dtype=jnp.int32)
    place, inner = (position // unit, position % unit)
    x = jnp.zeros_like(position) + lax.axis_index("gx")
    y = jnp.zeros_like(position) + lax.axis_index("gy")
    for number, (bit_x, bit_y, _) in enumerate(stages):
        leaves = 1 - (place >> (len(stages) - 1 - number)) % 2
        x = x ^ (leaves * bit_x)
        y = y ^ (leaves * bit_y)
    block = (x * size_y + y) * size_r + lax.axis_index("row")
    return (block * unit + inner)[:, None]


def halved(leaving, staying, flips, mesh_sizes):
    arrived = exchange(leaving, mesh_sizes, flips)
    half = staying.shape[0] // 2
    return staying[:half] + arrived[:half], staying[half:] + arrived[half:]


def rest_halved(leaving, staying, stages, done, mesh_sizes):
    for number in range(done, len(stages) - 1):
        leaving, staying = halved(leaving, staying, stages[number], mesh_sizes)
    arrived = exchange(leaving, mesh_sizes, stages[-1])
    return staying + arrived


def gelu_pair(values):
    root = math.sqrt(2.0 / math.pi)
    square = values * values
    bend = jnp.tanh(values * (root + (root * 0.044715) * square))
    cdf = 0.5 + 0.5 * bend
    value = values * cdf
    return value, cdf + (value - value * cdf) * (2.0 * root + (6.0 * root * 0.044715) * square)


def gelu_value(values):
    root = math.sqrt(2.0 / math.pi)
    return values * (0.5 + 0.5 * jnp.tanh(values * (root + (root * 0.044715) * (values * values))))


def product(left, right):
    return jnp.dot(left, right, preferred_element_type=jnp.float32)


def product_transposed(left, right):
    return lax.dot_general(left, right, (((1,), (1,)), ((), ())), preferred_element_type=jnp.float32)


def transposed_choice(rows, source):
    columns = lax.broadcasted_iota(jnp.int32, (rows.shape[0], source.shape[1]), 1)
    choice = jnp.where(columns == rows, 1.0, 0.0).astype(jnp.bfloat16)
    return product_transposed(choice, source).astype(jnp.bfloat16)


def column_tiles(width):
    tile = 256 if width % 256 == 0 else width
    return [slice(start, start + tile) for start in range(0, width, tile)]


def store_halves(value, columns, leaving_ref, staying_ref):
    half = value.shape[0] // 2
    leaving_ref[:, columns] = value[:half]
    staying_ref[:, columns] = value[half:]


def activated(left, weight, value_ref, slope_ref):
    tiles = column_tiles(value_ref.shape[1])
    ahead = product(left, weight[:, tiles[0]])
    for number, columns in enumerate(tiles):
        now = ahead
        if number + 1 < len(tiles):
            ahead = product(left, weight[:, tiles[number + 1]])
        value, slope = gelu_pair(now)
        value_ref[:, columns] = value.astype(jnp.bfloat16)
        slope_ref[:, columns] = slope


def forward_one_body(own_ref, a_ref, b_ref, c_ref, first_ref, middle_ref,
                     x_ref, h1_ref, s1_ref, h2_ref, s2_ref):
    count = own_ref.shape[0]
    for number, part in enumerate((own_ref, a_ref, b_ref, c_ref)):
        x_ref[number * count:(number + 1) * count, :] = part[...]
    activated(x_ref[...], first_ref, h1_ref, s1_ref)
    activated(h1_ref[...], middle_ref, h2_ref, s2_ref)


def forward_two_body(h2_ref, own_ref, a_ref, b_ref, c_ref, rows_ref, error_ref, leaving_ref, staying_ref):
    count = own_ref.shape[0]
    for number, part in enumerate((own_ref, a_ref, b_ref, c_ref)):
        error_ref[number * count:(number + 1) * count, :] = part[...]
    chosen = transposed_choice(rows_ref[...], h2_ref[...])
    for columns in column_tiles(error_ref.shape[1]):
        store_halves(product(chosen, error_ref[:, columns]), columns, leaving_ref, staying_ref)


def backward_body(carried_ref, weight_ref, slope_ref, source_ref, rows_ref, back_ref, leaving_ref, staying_ref):
    carried = carried_ref[...]
    for columns in column_tiles(back_ref.shape[1]):
        value = product_transposed(carried, weight_ref[columns, :]) * slope_ref[:, columns]
        back_ref[:, columns] = value.astype(jnp.bfloat16)
    chosen = transposed_choice(rows_ref[...], source_ref[...])
    for columns in column_tiles(back_ref.shape[1]):
        store_halves(product(chosen, back_ref[:, columns]), columns, leaving_ref, staying_ref)


def tied(value, *others):
    return lax.optimization_barrier((value, *others))[0]


def kernel_call(body, outputs, scratch=(), flops=1 << 31, far=(), far_outputs=(), copies=0):
    def call(*inputs):
        near, away = (pl.BlockSpec(memory_space=pltpu.VMEM), pl.BlockSpec(memory_space=pltpu.HBM))
        result = pl.pallas_call(
            body,
            cost_estimate=pl.CostEstimate(flops=flops, transcendentals=0, bytes_accessed=0),
            in_specs=[away if number in far else near for number in range(len(inputs))],
            out_specs=[away if number in far_outputs else near for number in range(len(outputs))],
            out_shape=[(pltpu.HBM if number in far_outputs else jax.ShapeDtypeStruct)(shape, dtype)
                       for number, (shape, dtype) in enumerate(outputs)],
            scratch_shapes=[pltpu.VMEM(shape, dtype) for shape, dtype in scratch]
            + [pltpu.SemaphoreType.DMA((copies,))] * (copies > 0),
            compiler_params=pltpu.CompilerParams(vmem_limit_bytes=VMEM_LIMIT),
        )(*(pltpu.with_memory_space_constraint(array, pltpu.HBM) if number in far else array
            for number, array in enumerate(inputs)))
        return result

    return call


def all_steps(concentrations, diffusivity, weight_first, weight_middle, weight_last):
    mesh_sizes = tuple(lax.axis_size(axis) for axis in ("gx", "gy", "row"))
    length, height, width = diffusivity.shape
    f32, bf16 = (jnp.float32, jnp.bfloat16)
    planes, rows = (length + 2 * HALO, height + 2 * EDGE)
    fixed = ((2, planes, rows, width), f32)
    buffers = [((planes, 8 + rows + 8, width), f32)] * 8 + [((planes, rows, width), f32)]
    buffers += [((whole_tiles((strips_of(planes, width)[1] + 1) * rows), width), f32)] * 2
    count = length * height * width // PATCH ** 3
    cells, hidden = weight_first.shape
    hidden_second = weight_middle.shape[1]
    total = 4 * count
    rows_first, rows_middle, rows_last = [chosen_rows(size, mesh_sizes) for size in (cells, hidden, hidden_second)]
    half_of = lambda chosen, width: ((chosen.shape[0] // 2, width), f32)
    stages = reduction_stages(mesh_sizes)
    big = 1 << 32

    layers = ((PACKED, height, width), bf16)
    face, face_third = (((2, HALO, height, width), f32), ((HALO - 1, height, width), f32))
    leading, trailing = kernel_call(
        first_faces_body, [layers, layers], scratch=[face, face, face_third, face_third], far=(0, 1), copies=4
    )(concentrations, diffusivity)
    before, after = x_halos(leading, trailing)
    brought = (concentrations, diffusivity, weight_last)
    near_state, near_third, near_last = kernel_call(
        bring_body, [(array.shape, array.dtype) for array in brought], far=(0, 1, 2), copies=3
    )(*brought)
    leading, trailing = edge_rows(near_state, near_third, before, after)
    below, above = y_halos(leading, trailing)
    whole, strips = assemble(near_state, near_third, before, after, below, above)
    state, inputs, targets, diffusivity_fixed = kernel_call(
        functools.partial(first_steps_body, PATCH),
        [(concentrations.shape, f32), ((count, cells), bf16), ((count, cells), bf16), fixed],
        scratch=buffers + [((length * height, width), f32)],
        far_outputs=(3,), copies=2,
    )(whole, *z_strips(strips))

    gather = lambda array: [exchange(array, mesh_sizes, flips) for flips in ((0, 0, 1), (0, 1, 0), (0, 1, 1))]
    all_inputs = gather(inputs)
    field, own_error = kernel_call(
        functools.partial(own_forward_body, PATCH, 1.0 / count), [(diffusivity.shape, f32), ((count, cells), bf16)],
        flops=big // 4,
    )(
        inputs, targets, weight_first, weight_middle, near_last
    )
    all_errors = gather(own_error)
    leading, trailing = kernel_call(store_faces, [layers, layers])(state, field)
    before, after = x_halos(leading, trailing)
    x, h1, s1, h2, s2 = kernel_call(
        forward_one_body,
        [((total, cells), bf16), ((total, hidden), bf16), ((total, hidden), f32), ((total, hidden_second), bf16),
         ((total, hidden_second), f32)],
        flops=big,
    )(tied(inputs, leading, trailing), *all_inputs, weight_first, weight_middle)
    leading, trailing = edge_rows(state, field, tied(before, h2), after)
    below, above = y_halos(leading, trailing)
    error, *last = kernel_call(
        forward_two_body, [((total, cells), bf16), half_of(rows_last, cells), half_of(rows_last, cells)], flops=big
    )(tied(h2, leading, trailing), own_error, *all_errors, rows_last)
    last = halved(*last, stages[0], mesh_sizes)
    back_second, *middle = kernel_call(
        backward_body,
        [((total, hidden_second), bf16), half_of(rows_middle, hidden_second), half_of(rows_middle, hidden_second)],
        flops=big // 2,
    )(error, weight_last, s2, h1, rows_middle)
    middle = halved(*middle, stages[0], mesh_sizes)
    last_leaving = last[0]
    whole, strips = assemble(state, field, before, after, tied(below, back_second, last_leaving, middle[0]), above)
    last = halved(*last, stages[1], mesh_sizes)
    back_first, *first = kernel_call(
        backward_body,
        [((total, hidden), bf16), half_of(rows_first, hidden), half_of(rows_first, hidden)],
        flops=big // 2,
    )(tied(back_second, strips), weight_middle, s1, x, rows_first)
    first = halved(*first, stages[0], mesh_sizes)
    middle = halved(*middle, stages[1], mesh_sizes)
    (state,) = kernel_call(last_steps_body, [(state.shape, f32)], scratch=buffers + [(state.shape, f32)],
                           flops=big, far_outputs=(0,), copies=4 if length % 4 == 0 else 1)(
        tied(whole, first[0], middle[0], last[0]), *z_strips(strips), diffusivity_fixed
    )
    grads = [rest_halved(*part, stages, done, mesh_sizes) for part, done in ((first, 1), (middle, 2), (last, 2))]
    return (state, *grads)


def solution(mesh):
    in_specs = (P(None, "gx", "gy", "row"), P("gx", "gy", "row"), P(), P(), P())
    out_specs = (
        P(None, "gx", "gy", "row"),
        P(("gx", "gy", "row"), None),
        P(("gx", "gy", "row"), None),
        P(("gx", "gy", "row"), None),
    )
    return jax.shard_map(all_steps, mesh=mesh, in_specs=in_specs, out_specs=out_specs, check_vma=False)
```

```python
import functools
import math

import jax
import jax.numpy as jnp
from jax import lax
from jax.experimental import pallas as pl
from jax.experimental.pallas import tpu as pltpu
from jax.sharding import PartitionSpec as P

STEPS = 6
PATCH = 8
HALO = STEPS // 2
EDGE = 4
AXES = ("gx", "gy", "row")
VMEM_LIMIT = 20 << 20


def ring(array, axis, distance):
    size = lax.axis_size(axis)
    return lax.ppermute(array, axis, [(i, (i + distance) % size) for i in range(size)])


def react(activator, inhibitor, diffusivity, lap_activator, lap_inhibitor, forcing):
    product = activator * inhibitor * inhibitor
    inner = diffusivity * lap_activator - product + 0.04 * (1.0 - activator)
    new_activator = activator + 0.1 * (inner if forcing is None else inner + forcing)
    new_inhibitor = inhibitor + 0.1 * (
        0.5 * diffusivity * lap_inhibitor + product - 0.1 * inhibitor
    )
    return (new_activator, new_inhibitor)


def fields(state, third):
    return ((lambda x, rows: state[0, x, rows, :], HALO), (lambda x, rows: state[1, x, rows, :], HALO),
            (lambda x, rows: third[x, rows, :], HALO - 1))


LAYERS = 3 * HALO - 1
PACKED = LAYERS + 2


def rounded(value):
    return value.astype(jnp.bfloat16).astype(jnp.float32)


def whole_tiles(rows):
    return -(-rows // 16) * 16


def plane_of(state, third, before, after, kind, plane, rows):
    read, depth = fields(state, third)[kind]
    length = state.shape[1]
    x = plane - HALO
    if x < -depth or x >= length + depth:
        return None
    if 0 <= x < length:
        return read(x, rows)
    halo, layer = (before, kind * HALO + depth + x) if x < 0 else (after, kind * HALO + x - length)
    value = halo[layer].astype(jnp.float32)
    if kind < 2 and x in (-1, length):
        value = value + halo[LAYERS + kind].astype(jnp.float32)
    return value[rows]


def edge_rows_body(state, third, before, after, leading_ref, trailing_ref, leading, trailing):
    length, height, width = state.shape[1:]
    planes = length + 2 * HALO
    for side, start_of, nearest in ((leading, lambda depth: 0, 0), (trailing, lambda depth: height - depth, HALO - 1)):
        for plane in range(planes):
            for kind, depth in enumerate((HALO, HALO, HALO - 1)):
                start, place = (start_of(depth), plane * PACKED)
                value = plane_of(state, third, before, after, kind, plane, slice(start, start + depth))
                if value is None:
                    value = jnp.zeros((depth, width), jnp.float32)
                side[place + kind * HALO:place + kind * HALO + depth, :] = value
                if kind < 2:
                    edge = value[nearest:nearest + 1]
                    side[place + LAYERS + kind:place + LAYERS + kind + 1, :] = edge - rounded(edge)
        filled = planes * PACKED
        if filled < side.shape[0]:
            side[filled:, :] = jnp.zeros((side.shape[0] - filled, width), jnp.float32)
    leading_ref[...] = leading[...].astype(jnp.bfloat16)
    trailing_ref[...] = trailing[...].astype(jnp.bfloat16)


def strips_of(planes, width):
    each = width // (2 * HALO)
    places = {}
    for kind in range(3):
        for plane in range(kind // 2, planes - kind // 2):
            number = len(places)
            places[kind, plane] = (number // each, (number % each) * 2 * HALO)
    return places, -(-len(places) // each)


def assemble_body(state, third, before, after, below_ref, above_ref, whole_ref, strips_ref, below, above, strips):
    _, height, width = state.shape[1:]
    planes, rows = whole_ref.shape[1:3]
    places, count = strips_of(planes, width)
    lanes = lax.broadcasted_iota(jnp.int32, (rows, width), 1)
    below[...] = below_ref[...].astype(jnp.float32)
    above[...] = above_ref[...].astype(jnp.float32)
    tiles = {}

    def gather_lanes(tile, value, shift, first, size):
        turned = pltpu.roll(value, shift, axis=1)
        here = (lanes >= first) & (lanes < first + size)
        tiles[tile] = jnp.where(here, turned, tiles[tile]) if tile in tiles else turned

    for kind, depth in enumerate((HALO, HALO, HALO - 1)):
        for plane in range(planes):
            value = plane_of(state, third, before, after, kind, plane, slice(0, height))
            if value is None:
                continue
            held = slice(plane * PACKED + kind * HALO, plane * PACKED + kind * HALO + depth)
            whole_ref[kind, plane, EDGE:EDGE + height, :] = value
            whole_ref[kind, plane, EDGE - depth:EDGE, :] = below[held, :]
            whole_ref[kind, plane, EDGE + height:EDGE + height + depth, :] = above[held, :]
            if kind < 2:
                rest = slice(plane * PACKED + LAYERS + kind, plane * PACKED + LAYERS + kind + 1)
                whole_ref[kind, plane, EDGE - 1:EDGE, :] = below[held.stop - 1:held.stop, :] + below[rest, :]
                whole_ref[kind, plane, EDGE + height:EDGE + height + 1, :] = (
                    above[held.start:held.start + 1, :] + above[rest, :])
            tile, shift = places[kind, plane]
            value = whole_ref[kind, plane]
            gather_lanes(tile, value, (shift + HALO) % width, shift, 2 * HALO)
            if kind < 2:
                first = 2 * (kind * planes + plane)
                gather_lanes(count, value - rounded(value), first + 1, first, 2)
    for tile, value in tiles.items():
        strips[tile * rows:(tile + 1) * rows, :] = value
    filled = len(tiles) * rows
    if filled < strips.shape[0]:
        strips[filled:, :] = jnp.zeros((strips.shape[0] - filled, width), jnp.float32)
    strips_ref[...] = strips[...].astype(jnp.bfloat16)


def load_sides(whole, earlier, later, kind, target, first):
    planes, rows, width = whole.shape[1:]
    places, count = strips_of(planes, width)
    lanes = lax.broadcasted_iota(jnp.int32, (rows, width), 1)

    def both(tile, shift, size):
        held = slice(tile * rows, (tile + 1) * rows)
        after = (lanes >= shift + size) & (lanes < shift + 2 * size)
        return pltpu.roll(jnp.where(after, later[held, :], earlier[held, :]), (2 * width - shift - size) % width, axis=1)

    for plane in range(planes):
        if (kind, plane) not in places:
            continue
        value = both(*places[kind, plane], HALO)
        if kind < 2:
            rest = both(count, 2 * (kind * planes + plane), 1)
            value = value + jnp.where((lanes == 0) | (lanes == width - 1), rest, 0.0)
        target[plane, first:first + rows, :] = value


def one_step(source, target, fixed, planes, rows, sides, finished=None):
    def some_rows(plane, first):
        held, here = (slice(8 + first, 16 + first), slice(first, first + 8))
        around, centers = ([], [])
        for pair in source:
            summed, center = ([], [])
            for field in pair:
                middle = field[plane, held, :]
                total = -6.0 * middle + field[plane + 1, held, :] + field[plane - 1, held, :]
                summed.append(total + field[plane, 9 + first:17 + first, :] + field[plane, 7 + first:15 + first, :])
                center.append(middle)
            width = center[0].shape[1]
            lanes = lax.broadcasted_iota(jnp.int32, center[0].shape, 1)
            up = [pltpu.roll(value, 1, axis=1) for value in center]
            down = [pltpu.roll(value, width - 1, axis=1) for value in center]
            around.append([summed[n] + jnp.where(lanes == 0, up[1 - n], up[n])
                           + jnp.where(lanes == width - 1, down[1 - n], down[n]) for n in range(2)])
            centers.append(center)
        for n in range(2 if sides else 1):
            still = [pair[n][plane, here, :] for pair in fixed] + [None]
            new = react(centers[0][n], centers[1][n], still[0], around[0][n], around[1][n], still[1])
            for pair, value in zip(target, new):
                pair[n][plane, held, :] = value

    for plane in range(*planes):
        for first in range(0, rows, 8):
            some_rows(plane, first)
        if finished is not None:
            finished(plane, target)


def run_steps(whole, earlier, later, fixed, now, then, finished=None):
    planes, rows = whole.shape[1:3]
    for kind, pair in enumerate(now):
        load_sides(whole, earlier, later, kind, pair[1], 8)
        for plane in range(planes):
            pair[0][plane, 8:8 + rows, :] = whole[kind, plane]
    for step in range(HALO):
        one_step(now, then, fixed, (step + 1, planes - step - 1), rows, step < HALO - 1, finished if step == HALO - 1 else None)
        now, then = then, now
    return now[0][0], now[1][0]


def move_order(patches_z, edge):
    lanes = patches_z * edge
    row = lax.broadcasted_iota(jnp.int32, (lanes, lanes), 0)
    column = lax.broadcasted_iota(jnp.int32, (lanes, lanes), 1)
    return jnp.where((row % patches_z) * edge + row // patches_z == column, 1.0, 0.0).astype(jnp.bfloat16)


def cell_order(edge):
    cells = edge ** 3
    row = lax.broadcasted_iota(jnp.int32, (cells, cells), 0)
    column = lax.broadcasted_iota(jnp.int32, (cells, cells), 1)
    return jnp.where((row % (edge * edge)) * edge + row // (edge * edge) == column, 1.0, 0.0).astype(jnp.bfloat16)


def half_tiles(source, count, rows, by_lane):
    half = by_lane // 2
    lanes = lax.broadcasted_iota(jnp.int32, (rows, by_lane), 1)
    out = []
    for b in range(count[1]):
        tiles = []
        for a in range(0, count[0], 2):
            low, high = [source[n * rows:(n + 1) * rows, (b // 2) * by_lane:(b // 2 + 1) * by_lane] for n in (a, a + 1)]
            if b % 2 == 0:
                high = pltpu.roll(high, half, axis=1)
            else:
                low = pltpu.roll(low, half, axis=1)
            tiles.append(jnp.where(lanes < half, low, high))
        out.append(jnp.concatenate(tiles, axis=1))
    return jnp.concatenate(out, axis=0)


def cube_starts(shape, edge):
    extent_x, extent_y = shape
    return [(px * edge + ix, py * edge) for px in range(extent_x // edge) for py in range(extent_y // edge)
            for ix in range(edge)]


def exact_product(left, right):
    high = left.astype(jnp.bfloat16)
    low = (left - high.astype(jnp.float32)).astype(jnp.bfloat16)
    return product(high, right) + product(low, right)


def paired(refs):
    pairs = list(zip(refs[::2], refs[1::2]))
    return pairs[:2], pairs[2:]


def first_steps_body(edge, whole, earlier_ref, later_ref, state_ref, inputs_ref, targets_ref, fixed_ref, *scratch):
    *fields_now, side, earlier, later, column_ref, semaphores = scratch
    length, height, width = state_ref.shape[1:]
    earlier[...] = earlier_ref[...].astype(jnp.float32)
    later[...] = later_ref[...].astype(jnp.float32)
    load_sides(whole, earlier, later, 2, side, 0)
    copies = start_copies([(whole.at[2], fixed_ref.at[0]), (side, fixed_ref.at[1])], semaphores)
    now = run_steps(whole, earlier, later, [(whole.at[2], side)], *paired(fields_now))
    move, order = (move_order(width // edge, edge), cell_order(edge))
    for species, (field, out_ref) in enumerate(zip(now, (inputs_ref, targets_ref))):
        for x in range(length):
            state_ref[species, x] = field[x + HALO, 8 + EDGE:8 + EDGE + height, :]
        for number, (x, y) in enumerate(cube_starts((length, height), edge)):
            column_ref[number * edge:(number + 1) * edge, :] = state_ref[species, x, y:y + edge, :]
        turned = product_transposed(move, column_ref[...].astype(jnp.bfloat16))
        columns = length * height // (edge * edge)
        cubes = half_tiles(turned, (edge, columns), width // edge, 2 * edge * edge)
        out_ref[...] = product(cubes.astype(jnp.bfloat16), order).astype(jnp.bfloat16)
    for copy in copies:
        copy.wait()


def own_forward_body(edge, scale, inputs_ref, targets_ref, first_ref, middle_ref, last_ref, field_ref, error_ref):
    length, height, width = field_ref.shape
    h1 = gelu_value(product(inputs_ref[...], first_ref[...])).astype(jnp.bfloat16)
    h2 = gelu_value(product(h1, middle_ref[...])).astype(jnp.bfloat16)
    forcing = product(h2, last_ref[...])
    error_ref[...] = ((forcing - targets_ref[...].astype(jnp.float32)) * scale).astype(jnp.bfloat16)
    cells = lax.broadcasted_iota(jnp.int32, (edge ** 3, edge ** 3), 1)
    row = lax.broadcasted_iota(jnp.int32, (edge ** 3, edge ** 3), 0)
    square = edge * edge
    order = jnp.where((cells % square) * edge + cells // square == row, 1.0, 0.0).astype(jnp.bfloat16)
    columns = length * height // square
    turned = half_tiles(exact_product(forcing, order), (columns, edge), width // edge, 2 * square)
    moved = exact_product(turned.T, move_order(width // edge, edge))
    for number, (x, y) in enumerate(cube_starts((length, height), edge)):
        field_ref[x, y:y + edge, :] = moved[number * edge:(number + 1) * edge, :]


def last_steps_body(whole, earlier_ref, later_ref, fixed, state_ref, *scratch):
    *fields_now, side, earlier, later, near, semaphores = scratch
    length, height, _ = state_ref.shape[1:]
    group = length // semaphores.shape[0]
    copies = []

    def finished(plane, pairs):
        x = plane - HALO
        for species, pair in enumerate(pairs):
            near[species, x] = pair[0][plane, 8 + EDGE:8 + EDGE + height, :]
        if (x + 1) % group == 0:
            held = slice(x + 1 - group, x + 1)
            copies.append(pltpu.make_async_copy(near.at[:, held], state_ref.at[:, held], semaphores.at[x // group]))
            copies[-1].start()

    earlier[...] = earlier_ref[...].astype(jnp.float32)
    later[...] = later_ref[...].astype(jnp.float32)
    load_sides(whole, earlier, later, 2, side, 0)
    both = [(fixed.at[0], fixed.at[1]), (whole.at[2], side)]
    run_steps(whole, earlier, later, both, *paired(fields_now), finished)
    for copy in copies:
        copy.wait()


def start_copies(pairs, semaphores):
    copies = [pltpu.make_async_copy(*pair, semaphores.at[number]) for number, pair in enumerate(pairs)]
    for copy in copies:
        copy.start()
    return copies


def bring_body(*refs):
    count = len(refs) // 2
    for copy in start_copies(zip(refs[:count], refs[count:-1]), refs[-1]):
        copy.wait()


def store_faces(state, third, leading_ref, trailing_ref):
    length = third.shape[0]
    for kind, depth in enumerate((HALO, HALO, HALO - 1)):
        read = fields(state, third)[kind][0]
        for plane in range(depth):
            for out_ref, x, nearest in ((leading_ref, plane, 0), (trailing_ref, length - depth + plane, length - 1)):
                value = read(x, slice(None))
                out_ref[kind * HALO + plane] = value.astype(jnp.bfloat16)
                if kind < 2 and x == nearest:
                    out_ref[LAYERS + kind] = (value - rounded(value)).astype(jnp.bfloat16)


def first_faces_body(state_ref, third_ref, leading_ref, trailing_ref, low, high, low_third, high_third, semaphores):
    length = third_ref.shape[0]
    for copy in start_copies((
        (state_ref.at[:, :HALO], low), (state_ref.at[:, length - HALO:], high),
        (third_ref.at[:HALO - 1], low_third), (third_ref.at[length - HALO + 1:], high_third),
    ), semaphores):
        copy.wait()
    for kind, depth in enumerate((HALO, HALO, HALO - 1)):
        for out_ref, near, third, nearest in ((leading_ref, low, low_third, 0), (trailing_ref, high, high_third, depth - 1)):
            for plane in range(depth):
                value = near[kind, plane] if kind < 2 else third[plane]
                out_ref[kind * HALO + plane] = value.astype(jnp.bfloat16)
                if kind < 2 and plane == nearest:
                    out_ref[LAYERS + kind] = (value - rounded(value)).astype(jnp.bfloat16)


def x_halos(leading, trailing):
    return ring(trailing, "gx", 1), ring(leading, "gx", -1)


def edge_rows(state, third, before, after):
    planes = state.shape[1] + 2 * HALO
    packed = (whole_tiles(planes * PACKED), state.shape[3])
    return kernel_call(edge_rows_body, [(packed, jnp.bfloat16)] * 2, scratch=[(packed, jnp.float32)] * 2)(
        state, third, before, after
    )


def y_halos(leading, trailing):
    return ring(trailing, "gy", 1), ring(leading, "gy", -1)


def assemble(state, third, before, after, below, above):
    length, height, width = state.shape[1:]
    planes, rows = (length + 2 * HALO, height + 2 * EDGE)
    strips = (whole_tiles((strips_of(planes, width)[1] + 1) * rows), width)
    outputs = [((3, planes, rows, width), jnp.float32), (strips, jnp.bfloat16)]
    scratch = [(shape, jnp.float32) for shape in (below.shape, above.shape, strips)]
    return kernel_call(assemble_body, outputs, scratch=scratch)(
        state, third, before, after, below, above
    )


def z_strips(strips):
    earlier = ring(strips, "row", 1)
    return earlier, (earlier if lax.axis_size("row") == 2 else ring(strips, "row", -1))


def exchange(array, mesh_sizes, flips):
    size_x, size_y, size_r = mesh_sizes
    route = []
    for i in range(size_x):
        for j in range(size_y):
            for k in range(size_r):
                here = (i * size_y + j) * size_r + k
                there = ((i ^ flips[0]) * size_y + (j ^ flips[1])) * size_r + (k ^ flips[2])
                route.append((here, there))
    return lax.ppermute(array, AXES, route)


def reduction_stages(mesh_sizes):
    size_x, size_y, _ = mesh_sizes
    stages = []
    bit = 1
    while bit < size_x:
        stages.append((bit, 0, 0))
        bit *= 2
    bit = 2
    while bit < size_y:
        stages.append((0, bit, 0))
        bit *= 2
    return stages


def chosen_rows(total, mesh_sizes):
    size_x, size_y, size_r = mesh_sizes
    stages = reduction_stages(mesh_sizes)
    unit = total // (size_x * size_y * size_r)
    blocks = 1 << len(stages)
    position = jnp.arange(blocks * unit, dtype=jnp.int32)
    place, inner = (position // unit, position % unit)
    x = jnp.zeros_like(position) + lax.axis_index("gx")
    y = jnp.zeros_like(position) + lax.axis_index("gy")
    for number, (bit_x, bit_y, _) in enumerate(stages):
        leaves = 1 - (place >> (len(stages) - 1 - number)) % 2
        x = x ^ (leaves * bit_x)
        y = y ^ (leaves * bit_y)
    block = (x * size_y + y) * size_r + lax.axis_index("row")
    return (block * unit + inner)[:, None]


def halved(leaving, staying, flips, mesh_sizes):
    arrived = exchange(leaving, mesh_sizes, flips)
    half = staying.shape[0] // 2
    return staying[:half] + arrived[:half], staying[half:] + arrived[half:]


def rest_halved(leaving, staying, stages, done, mesh_sizes):
    for number in range(done, len(stages) - 1):
        leaving, staying = halved(leaving, staying, stages[number], mesh_sizes)
    arrived = exchange(leaving, mesh_sizes, stages[-1])
    return staying + arrived


def gelu_pair(values):
    root = math.sqrt(2.0 / math.pi)
    square = values * values
    bend = jnp.tanh(values * (root + (root * 0.044715) * square))
    cdf = 0.5 + 0.5 * bend
    value = values * cdf
    return value, cdf + (value - value * cdf) * (2.0 * root + (6.0 * root * 0.044715) * square)


def gelu_value(values):
    root = math.sqrt(2.0 / math.pi)
    return values * (0.5 + 0.5 * jnp.tanh(values * (root + (root * 0.044715) * (values * values))))


def product(left, right):
    return jnp.dot(left, right, preferred_element_type=jnp.float32)


def product_transposed(left, right):
    return lax.dot_general(left, right, (((1,), (1,)), ((), ())), preferred_element_type=jnp.float32)


def transposed_choice(rows, source):
    columns = lax.broadcasted_iota(jnp.int32, (rows.shape[0], source.shape[1]), 1)
    choice = jnp.where(columns == rows, 1.0, 0.0).astype(jnp.bfloat16)
    return product_transposed(choice, source).astype(jnp.bfloat16)


def column_tiles(width):
    tile = 256 if width % 256 == 0 else width
    return [slice(start, start + tile) for start in range(0, width, tile)]


def store_halves(value, columns, leaving_ref, staying_ref):
    half = value.shape[0] // 2
    leaving_ref[:, columns] = value[:half]
    staying_ref[:, columns] = value[half:]


def activated(left, weight, value_ref, slope_ref):
    tiles = column_tiles(value_ref.shape[1])
    ahead = product(left, weight[:, tiles[0]])
    for number, columns in enumerate(tiles):
        now = ahead
        if number + 1 < len(tiles):
            ahead = product(left, weight[:, tiles[number + 1]])
        value, slope = gelu_pair(now)
        value_ref[:, columns] = value.astype(jnp.bfloat16)
        slope_ref[:, columns] = slope


def forward_one_body(own_ref, a_ref, b_ref, c_ref, first_ref, middle_ref,
                     x_ref, h1_ref, s1_ref, h2_ref, s2_ref):
    count = own_ref.shape[0]
    for number, part in enumerate((own_ref, a_ref, b_ref, c_ref)):
        x_ref[number * count:(number + 1) * count, :] = part[...]
    activated(x_ref[...], first_ref, h1_ref, s1_ref)
    activated(h1_ref[...], middle_ref, h2_ref, s2_ref)


def forward_two_body(h2_ref, own_ref, a_ref, b_ref, c_ref, rows_ref, error_ref, leaving_ref, staying_ref):
    count = own_ref.shape[0]
    for number, part in enumerate((own_ref, a_ref, b_ref, c_ref)):
        error_ref[number * count:(number + 1) * count, :] = part[...]
    chosen = transposed_choice(rows_ref[...], h2_ref[...])
    for columns in column_tiles(error_ref.shape[1]):
        store_halves(product(chosen, error_ref[:, columns]), columns, leaving_ref, staying_ref)


def backward_body(carried_ref, weight_ref, slope_ref, source_ref, rows_ref, back_ref, leaving_ref, staying_ref):
    carried = carried_ref[...]
    for columns in column_tiles(back_ref.shape[1]):
        value = product_transposed(carried, weight_ref[columns, :]) * slope_ref[:, columns]
        back_ref[:, columns] = value.astype(jnp.bfloat16)
    chosen = transposed_choice(rows_ref[...], source_ref[...])
    for columns in column_tiles(back_ref.shape[1]):
        store_halves(product(chosen, back_ref[:, columns]), columns, leaving_ref, staying_ref)


def tied(value, *others):
    return lax.optimization_barrier((value, *others))[0]


def kernel_call(body, outputs, scratch=(), flops=1 << 31, far=(), far_outputs=(), copies=0):
    def call(*inputs):
        near, away = (pl.BlockSpec(memory_space=pltpu.VMEM), pl.BlockSpec(memory_space=pltpu.HBM))
        result = pl.pallas_call(
            body,
            cost_estimate=pl.CostEstimate(flops=flops, transcendentals=0, bytes_accessed=0),
            in_specs=[away if number in far else near for number in range(len(inputs))],
            out_specs=[away if number in far_outputs else near for number in range(len(outputs))],
            out_shape=[(pltpu.HBM if number in far_outputs else jax.ShapeDtypeStruct)(shape, dtype)
                       for number, (shape, dtype) in enumerate(outputs)],
            scratch_shapes=[pltpu.VMEM(shape, dtype) for shape, dtype in scratch]
            + [pltpu.SemaphoreType.DMA((copies,))] * (copies > 0),
            compiler_params=pltpu.CompilerParams(vmem_limit_bytes=VMEM_LIMIT),
        )(*(pltpu.with_memory_space_constraint(array, pltpu.HBM) if number in far else array
            for number, array in enumerate(inputs)))
        return result

    return call


def all_steps(concentrations, diffusivity, weight_first, weight_middle, weight_last):
    mesh_sizes = tuple(lax.axis_size(axis) for axis in AXES)
    length, height, width = diffusivity.shape
    f32, bf16 = (jnp.float32, jnp.bfloat16)
    planes, rows = (length + 2 * HALO, height + 2 * EDGE)
    fixed = ((2, planes, rows, width), f32)
    buffers = [((planes, 8 + rows + 8, width), f32)] * 8 + [((planes, rows, width), f32)]
    buffers += [((whole_tiles((strips_of(planes, width)[1] + 1) * rows), width), f32)] * 2
    count = length * height * width // PATCH ** 3
    cells, hidden = weight_first.shape
    hidden_second = weight_middle.shape[1]
    total = 4 * count
    rows_first, rows_middle, rows_last = [chosen_rows(size, mesh_sizes) for size in (cells, hidden, hidden_second)]
    half_of = lambda chosen, width: ((chosen.shape[0] // 2, width), f32)
    stages = reduction_stages(mesh_sizes)
    big = 1 << 32

    layers = ((PACKED, height, width), bf16)
    face, face_third = (((2, HALO, height, width), f32), ((HALO - 1, height, width), f32))
    leading, trailing = kernel_call(
        first_faces_body, [layers, layers], scratch=[face, face, face_third, face_third], far=(0, 1), copies=4
    )(concentrations, diffusivity)
    before, after = x_halos(leading, trailing)
    brought = (concentrations, diffusivity, weight_last)
    near_state, near_third, near_last = kernel_call(
        bring_body, [(array.shape, array.dtype) for array in brought], far=(0, 1, 2), copies=3
    )(*brought)
    leading, trailing = edge_rows(near_state, near_third, before, after)
    below, above = y_halos(leading, trailing)
    whole, strips = assemble(near_state, near_third, before, after, below, above)
    state, inputs, targets, diffusivity_fixed = kernel_call(
        functools.partial(first_steps_body, PATCH),
        [(concentrations.shape, f32), ((count, cells), bf16), ((count, cells), bf16), fixed],
        scratch=buffers + [((length * height, width), f32)],
        far_outputs=(3,), copies=2,
    )(whole, *z_strips(strips))

    gather = lambda array: [exchange(array, mesh_sizes, flips) for flips in ((0, 0, 1), (0, 1, 0), (0, 1, 1))]
    all_inputs = gather(inputs)
    field, own_error = kernel_call(
        functools.partial(own_forward_body, PATCH, 1.0 / count), [(diffusivity.shape, f32), ((count, cells), bf16)],
        flops=big // 4,
    )(
        inputs, targets, weight_first, weight_middle, near_last
    )
    all_errors = gather(own_error)
    leading, trailing = kernel_call(store_faces, [layers, layers])(state, field)
    before, after = x_halos(leading, trailing)
    x, h1, s1, h2, s2 = kernel_call(
        forward_one_body,
        [((total, cells), bf16), ((total, hidden), bf16), ((total, hidden), f32), ((total, hidden_second), bf16),
         ((total, hidden_second), f32)],
        flops=big,
    )(tied(inputs, leading, trailing), *all_inputs, weight_first, weight_middle)
    leading, trailing = edge_rows(state, field, tied(before, h2), after)
    below, above = y_halos(leading, trailing)
    error, *last = kernel_call(
        forward_two_body, [((total, cells), bf16), half_of(rows_last, cells), half_of(rows_last, cells)], flops=big
    )(tied(h2, leading, trailing), own_error, *all_errors, rows_last)
    last = halved(*last, stages[0], mesh_sizes)
    back_second, *middle = kernel_call(
        backward_body,
        [((total, hidden_second), bf16), half_of(rows_middle, hidden_second), half_of(rows_middle, hidden_second)],
        flops=big // 2,
    )(error, weight_last, s2, h1, rows_middle)
    middle = halved(*middle, stages[0], mesh_sizes)
    last_leaving = last[0]
    whole, strips = assemble(state, field, before, after, tied(below, back_second, last_leaving, middle[0]), above)
    last = halved(*last, stages[1], mesh_sizes)
    back_first, *first = kernel_call(
        backward_body,
        [((total, hidden), bf16), half_of(rows_first, hidden), half_of(rows_first, hidden)],
        flops=big // 2,
    )(tied(back_second, strips), weight_middle, s1, x, rows_first)
    first = halved(*first, stages[0], mesh_sizes)
    middle = halved(*middle, stages[1], mesh_sizes)
    (state,) = kernel_call(last_steps_body, [(state.shape, f32)], scratch=buffers + [(state.shape, f32)],
                           flops=big, far_outputs=(0,), copies=4 if length % 4 == 0 else 1)(
        tied(whole, first[0], middle[0], last[0]), *z_strips(strips), diffusivity_fixed
    )
    grads = [rest_halved(*part, stages, done, mesh_sizes) for part, done in ((first, 1), (middle, 2), (last, 2))]
    return (state, *grads)


def solution(mesh):
    in_specs = (P(None, *AXES), P(*AXES), P(), P(), P())
    out_specs = (
        P(None, *AXES),
        P(AXES, None),
        P(AXES, None),
        P(AXES, None),
    )
    return jax.shard_map(all_steps, mesh=mesh, in_specs=in_specs, out_specs=out_specs, check_vma=False)
```
